512 devices in a mesh: orb: 32 (over z, core), grp: 16 (over y, x).
Axes of the slice: x: 4, y: 4, z: 16, core: 2. Of those that a mesh axis runs over, the one named last changes fastest.
Arguments:
- orbitals: bfloat16 [2048, 32, 1024], P('orb', 'grp'), may hold values from -6 to 6
- pair_list: int32 [32, 32, 3], replicated, may hold values from 0 to 63, as said below
- offsets: int32 [2048, 3], replicated, may hold values from 0 to 15
Outputs:
- exchange_action: float32 [2048, 32, 1024], P('orb', 'grp')
The draws below stay inside these ranges and needn't reach their ends.
Inputs may be any that keep to these rules, and one draw needn't show every extreme that they name: pair_list[o, r, 0] and pair_list[o, r, 1] are below 64; pair_list[o, r, 2] is a slot below 64, distinct within each block o, so a block names each owner group at most 2 times; in every draw some owner group is named 2 times by every block; the two orbitals of a pair differ.
All inputs are finite; a program needn't handle non-finite values.
Results may differ from the reference program's by a relative error of at most 0.0006.
Values may be sent and summed in bfloat16 or wider, within the bound.
No kernel may reach another device: no remote copies, remote signals or barrier semaphores. Data moves between devices by JAX's collectives and lax.ppermute only.
A program may use at most 64 MiB of HBM per device.

```python
import math
import jax
import jax.numpy as jnp
from jax import lax

BOX = 32
ORB_GRP = 64
CAP = 2
ORBITALS = 2048
N_ORB = 32


def draw_pair_list(key, part):
    slot_count = N_ORB * CAP
    keep_count = slot_count // 2
    base_key = jax.random.fold_in(key, 17)
    full_group = jax.random.randint(jax.random.fold_in(base_key, 1), (), 0, N_ORB)
    slot_ids = jnp.arange(slot_count, dtype=jnp.int32)

    def one_block(block_num):
        block_key = jax.random.fold_in(base_key, block_num + 100)
        key_score, key_second, key_first, key_other = jax.random.split(block_key, 4)
        scores = jax.random.randint(key_score, (slot_count,), 0, 1 << 20) * slot_count + slot_ids
        scores = jnp.where(slot_ids // CAP == full_group, -1 - slot_ids, scores)
        chosen = jnp.argsort(scores, stable=True)[:keep_count].astype(jnp.int32)
        second_local = jax.random.randint(key_second, (keep_count,), 0, ORB_GRP)
        first_raw = jax.random.randint(key_first, (keep_count,), 0, ORB_GRP)
        other_local = (second_local + 1 + jax.random.randint(key_other, (keep_count,), 0, ORB_GRP - 1)) % ORB_GRP
        first_local = jnp.where(chosen // CAP == block_num, other_local, first_raw)
        return jnp.stack([second_local, first_local, chosen], axis=1)
    return jax.vmap(one_block)(jnp.arange(N_ORB, dtype=jnp.int32)).astype(jnp.int32)


def with_ends(values, own_key, least, largest):
    longest = values.shape.index(max(values.shape))
    spots = []
    for shift in (0, 1):
        where = [jax.random.randint(jax.random.fold_in(own_key, axis), (), 0, length) for axis, length in enumerate(values.shape)]
        where[longest] = (where[longest] + shift) % values.shape[longest]
        spots.append(tuple(where))
    return values.at[spots[0]].set(least).at[spots[1]].set(largest)


def level_of(stream_key, shape, cuts, low, top_value):
    gain = 1.0
    for position, parts in cuts:
        draws = jax.random.uniform(jax.random.fold_in(jax.random.fold_in(stream_key, 6), position), (parts,), jnp.float32, low / len(cuts), top_value / len(cuts))
        gain = gain * jnp.repeat(jnp.exp(draws), shape[position] // parts).reshape((-1,) + (1,) * (len(shape) - 1 - position))
    return gain


def noise(own_key, extent, spread, reach, cuts=(), held_as=jnp.bfloat16):
    result = jax.random.normal(own_key, extent, jnp.float32) * spread
    if len(cuts) > 0:
        result = level_of(own_key, extent, cuts, -0.22, 0.18) * result
    return jnp.clip(result, min=-reach, max=reach).astype(held_as)


def setup_inputs(seed: int = 0) -> dict:
    key_of = jax.random.split(jax.random.key(seed), 4)
    orbitals = noise(key_of[0], (ORBITALS, BOX, BOX * BOX), 1.0, 6.0, ((0, 32), (1, 16)))
    pair_list = draw_pair_list(jax.random.fold_in(key_of[3], 71), 0)
    offsets = with_ends(jax.random.randint(key_of[2], (ORBITALS, 3), 0, BOX // 2), jax.random.fold_in(key_of[2], 1), 0, (BOX // 2) - 1).astype(jnp.int32)
    return {"orbitals": orbitals, "pair_list": pair_list, "offsets": offsets}


screen_shift = 0.25
highest = lax.Precision.HIGHEST
shared_forms = ('ab,pbyz->payz', 'ab,pxbz->pxaz', 'ab,pxyb->pxya')
single_forms = ('pab,pbyz->payz', 'pab,pxbz->pxaz', 'pab,pxyb->pxya')

def sine_table(length):
    counts = jnp.arange(length).astype(jnp.float32) + 1.0
    return jnp.sqrt(2.0 / (length + 1.0)) * jnp.sin(math.pi * counts[:, None] * counts[None, :] / (length + 1.0))

def green_table(length):
    counts = jnp.arange(length).astype(jnp.float32) + 1.0
    levels = 2.0 - 2.0 * jnp.cos(math.pi * counts / (length + 1.0))
    return 1.0 / (levels[:, None, None] + levels[None, :, None] + levels[None, None, :] + screen_shift)

def shift_tables(displace, length):
    places = jnp.arange(length, dtype=jnp.int32)
    return (places[None, None, :] == places[None, :, None] + displace[:, None, None]).astype(jnp.float32)

def along_shared(table, field, dimension):
    return jnp.einsum(shared_forms[dimension], table, field, precision=highest)

def along_single(tables, field, dimension):
    return jnp.einsum(single_forms[dimension], tables, field, precision=highest)

def pair_terms(first_box, second_box, displace):
    length = first_box.shape[1]
    transform = sine_table(length)
    tables = [shift_tables(displace[:, axis_num], length) for axis_num in range(3)]
    shifted = second_box
    for dimension in range(3):
        shifted = along_single(tables[dimension], shifted, dimension)
    charge = first_box * shifted
    for dimension in range(3):
        charge = along_shared(transform, charge, dimension)
    charge = charge * green_table(length)[None]
    for dimension in range(3):
        charge = along_shared(transform, charge, dimension)
    to_first = charge * shifted
    returned = charge * first_box
    for dimension in range(3):
        returned = along_single(jnp.swapaxes(tables[dimension], 1, 2), returned, dimension)
    return (to_first, returned)

def reference(orbitals, pair_list, offsets):
    length = orbitals.shape[1]
    groups = pair_list.shape[0]

    def accumulate(summed, block_data):
        block_pairs, block_num = block_data
        second_ids = (block_num * ORB_GRP + block_pairs[:, 0]).astype(jnp.int32)
        first_ids = (block_pairs[:, 2] // CAP * ORB_GRP + block_pairs[:, 1]).astype(jnp.int32)
        displace = (offsets[second_ids] - offsets[first_ids]).astype(jnp.int32)
        first_box = orbitals[first_ids].astype(jnp.float32).reshape(-1, length, length, length)
        second_box = orbitals[second_ids].astype(jnp.float32).reshape(-1, length, length, length)
        to_first, returned = pair_terms(first_box, second_box, displace)
        summed = summed.at[first_ids].add(to_first.reshape(-1, length, length * length))
        summed = summed.at[second_ids].add(returned.reshape(-1, length, length * length))
        return (summed, None)
    initial = jnp.zeros(orbitals.shape, jnp.float32)
    summed, unused = lax.scan(accumulate, initial, (pair_list, jnp.arange(groups, dtype=jnp.int32)))
    return summed
```

```python
import functools
import math

import jax
import jax.numpy as jnp
from jax import lax
from jax.experimental import pallas as pl
from jax.experimental.pallas import tpu as pltpu
from jax.sharding import PartitionSpec as P

BOX = 32
PLANE = BOX * BOX
ORB_GRP = 64
CAP = 2
SCREEN = 0.25
LANES = 128
TOP_EXP = 14.0
highest = lax.Precision.HIGHEST


def sine_table():
    counts = jnp.arange(BOX).astype(jnp.float32) + 1.0
    return jnp.sqrt(2.0 / (BOX + 1.0)) * jnp.sin(
        math.pi * counts[:, None] * counts[None, :] / (BOX + 1.0)
    )


def green_rows():
    levels = 2.0 - 2.0 * jnp.cos(
        math.pi * (jnp.arange(BOX).astype(jnp.float32) + 1.0) / (BOX + 1.0)
    )
    lanes = jnp.arange(PLANE, dtype=jnp.int32)

    def level(index):
        return 2.0 - 2.0 * jnp.cos(math.pi * (index.astype(jnp.float32) + 1.0) / (BOX + 1.0))

    return 1.0 / (levels[:, None] + (level(lanes // BOX) + level(lanes % BOX))[None, :] + SCREEN)


def halves(value):
    high = value.astype(jnp.bfloat16)
    return high, (value - high.astype(jnp.float32)).astype(jnp.bfloat16)


def dot(a, b):
    return jnp.dot(a, b, preferred_element_type=jnp.float32)


def plane_kernel(sine_ref, high_ref, low_ref):
    lane = lax.broadcasted_iota(jnp.int32, (BOX, PLANE), 1)
    row = lax.broadcasted_iota(jnp.int32, (BOX, PLANE), 0)
    by_y = jnp.where((lane >> 5) == row, 1.0, 0.0).astype(jnp.bfloat16)
    by_z = jnp.where((lane & (BOX - 1)) == row, 1.0, 0.0).astype(jnp.bfloat16)
    sine = sine_ref[...]
    parts = []
    rest = sine
    for _ in range(3):
        piece = rest.astype(jnp.bfloat16)
        parts.append(piece)
        rest = rest - piece.astype(jnp.float32)
    cols_y = dot(parts[0], by_y) + dot(parts[1], by_y) + dot(parts[2], by_y)
    cols_z = dot(parts[0], by_z) + dot(parts[1], by_z) + dot(parts[2], by_z)
    for m in range(BOX):
        block = cols_y[m : m + 1, :] * cols_z
        high = block.astype(jnp.bfloat16)
        high_ref[pl.ds(m * BOX, BOX), :] = high
        low_ref[pl.ds(m * BOX, BOX), :] = (block - high.astype(jnp.float32)).astype(jnp.bfloat16)


def plane_tables(sine):
    shape = jax.ShapeDtypeStruct((PLANE, PLANE), jnp.bfloat16)
    return pl.pallas_call(plane_kernel, out_shape=(shape, shape), name="plane_tables")(sine)


def pair_kernel(
    share, moves_ref, boxes_ref, high_ref, low_ref, green_ref, sine_ref, out_ref, first, second
):
    depth = boxes_ref.shape[1]
    sides = BOX // depth
    rows = share * BOX
    for s in range(sides):
        for k in range(share):
            piece = boxes_ref[s * share + k].astype(jnp.float32)
            at = k * BOX + s * depth
            first[at : at + depth, :] = piece[:, :PLANE]
            second[at : at + depth, :] = piece[:, PLANE:]

    row = lax.broadcasted_iota(jnp.int32, (rows, rows), 0)
    col = lax.broadcasted_iota(jnp.int32, (rows, rows), 1)
    same = (row >> 5) == (col >> 5)
    step = jnp.zeros((rows, rows), jnp.int32)
    for k in range(share):
        step = jnp.where((row >> 5) == k, moves_ref[k, 0], step)
    ahead = jnp.where(same & (col == row + step), 1.0, 0.0).astype(jnp.bfloat16)
    back = jnp.where(same & (row == col + step), 1.0, 0.0).astype(jnp.bfloat16)

    lane = lax.broadcasted_iota(jnp.int32, (BOX, PLANE), 1)
    y, z = lane >> 5, lane & (BOX - 1)

    def moved(value, dy, dz):
        turned = pltpu.roll(value, (PLANE - (dy * BOX + dz)) & (PLANE - 1), 1)
        inside = (y + dy >= 0) & (y + dy < BOX) & (z + dz >= 0) & (z + dz < BOX)
        return jnp.where(inside, turned, 0.0)

    sine = sine_ref[...]
    wide = jnp.concatenate([jnp.concatenate([sine] * share, 1)] * share, 0)
    wide = jnp.where(same, wide, 0.0)
    sine_high, sine_low = halves(wide)
    sine_three = jnp.concatenate([sine_high, sine_high, sine_low], 1)

    def along_x(value):
        high, low = halves(value)
        return dot(sine_three, jnp.concatenate([high, low, high], 0))

    def along_plane(value):
        high, low = halves(value)
        both = dot(jnp.concatenate([high, low], 0), high_ref[...])
        return both[:rows] + both[rows:] + dot(high, low_ref[...])

    turned = [
        moved(second[k * BOX : (k + 1) * BOX, :], moves_ref[k, 1], moves_ref[k, 2])
        for k in range(share)
    ]
    shifted = dot(ahead, jnp.concatenate(turned, 0).astype(jnp.bfloat16))
    own = first[...]
    modes = along_plane(along_x(own * shifted))
    modes = modes * jnp.concatenate([green_ref[...]] * share, 0)
    potential = along_x(along_plane(modes))

    to_first = potential * shifted
    high, low = halves(potential * own)
    upright = dot(jnp.concatenate([back, back], 1), jnp.concatenate([high, low], 0))
    for k in range(share):
        part = slice(k * BOX, (k + 1) * BOX)
        returned = moved(upright[part], -moves_ref[k, 1], -moves_ref[k, 2])
        mine = to_first[part]
        peak = jnp.max(
            jnp.maximum(jnp.abs(mine), jnp.abs(returned)), axis=(0, 1), keepdims=True
        )
        power = jnp.floor(TOP_EXP - jnp.log2(jnp.maximum(peak, 1e-30)))
        gain = jnp.exp2(power)
        first[part, :] = mine * gain
        second[part, :] = returned * gain
        note = jnp.broadcast_to(power, (depth, LANES))
        for s in range(sides):
            at = k * BOX + s * depth
            out_ref[s * share + k, :, 0:PLANE] = first[at : at + depth, :]
            out_ref[s * share + k, :, PLANE : PLANE + LANES] = note
            out_ref[s * share + k, :, PLANE + LANES :] = second[at : at + depth, :]


def pair_terms(boxes, moves, high, low, green, sine):
    rows, depth, _ = boxes.shape
    share = moves.shape[0]
    vmem = pl.BlockSpec(memory_space=pltpu.VMEM)
    return pl.pallas_call(
        functools.partial(pair_kernel, share),
        out_shape=jax.ShapeDtypeStruct((rows, depth, 2 * PLANE + LANES), jnp.float32),
        in_specs=[pl.BlockSpec(memory_space=pltpu.SMEM)] + [vmem] * 5,
        out_specs=vmem,
        scratch_shapes=[pltpu.VMEM((share * BOX, PLANE), jnp.float32)] * 2,
        name="pair_terms",
    )(moves, boxes, high, low, green, sine)


def per_device(orbitals, pair_list, offsets):
    groups = lax.axis_size("orb")
    layers = lax.axis_size("grp")
    me = lax.axis_index("orb")
    region = lax.axis_index("grp")
    held, depth, plane = orbitals.shape
    slot_count = groups * CAP
    pair_count = pair_list.shape[1]
    share = pair_count // layers

    wanted = me * CAP + jnp.arange(CAP, dtype=jnp.int32)
    asked = pair_list[:, None, :, 2] == wanted[None, :, None]
    asked_valid = jnp.any(asked, axis=2).reshape(slot_count)
    asked_local = jnp.sum(jnp.where(asked, pair_list[:, None, :, 1], 0), axis=2)
    asked_local = asked_local.reshape(slot_count)
    incoming = lax.all_to_all(
        jnp.take(orbitals, asked_local, axis=0), "orb", split_axis=0, concat_axis=0, tiled=True
    )

    own = lax.dynamic_index_in_dim(pair_list, me, 0, keepdims=False)
    first_local, second_local, slot = own[:, 0], own[:, 1], own[:, 2]
    rows = jnp.concatenate(
        [jnp.take(incoming, slot, axis=0), jnp.take(orbitals, first_local, axis=0)], axis=2
    )
    boxes = lax.all_to_all(rows, "grp", split_axis=0, concat_axis=0, tiled=True)

    part = lax.dynamic_slice_in_dim(own, region * share, share, 0)
    first_ids = me * ORB_GRP + part[:, 0]
    second_ids = part[:, 2] // CAP * ORB_GRP + part[:, 1]
    moves = jnp.take(offsets, first_ids, axis=0) - jnp.take(offsets, second_ids, axis=0)

    sine = sine_table()
    high, low = plane_tables(sine)
    terms = pair_terms(boxes, moves, high, low, green_rows(), sine).astype(jnp.float16)
    terms = lax.all_to_all(terms, "grp", split_axis=0, concat_axis=0, tiled=True)

    slot_hot = slot[None, :] == jnp.arange(slot_count, dtype=jnp.int32)[:, None]
    row_of_slot = jnp.sum(
        jnp.where(slot_hot, jnp.arange(pair_count, dtype=jnp.int32)[None, :], 0), axis=1
    )
    to_first = lax.all_to_all(
        jnp.take(terms[:, :, : plane + LANES], row_of_slot, axis=0),
        "orb",
        split_axis=0,
        concat_axis=0,
        tiled=True,
    )

    local_ids = jnp.arange(held, dtype=jnp.int32)[:, None]
    kept_gain = jnp.exp2(-terms[:, 0, plane].astype(jnp.float32))
    kept_hot = jnp.where(first_local[None, :] == local_ids, kept_gain[None, :], 0.0)
    back_gain = jnp.exp2(-to_first[:, 0, plane].astype(jnp.float32))
    back_hot = jnp.where(
        (asked_local[None, :] == local_ids) & asked_valid[None, :], back_gain[None, :], 0.0
    )
    kept = terms[:, :, plane + LANES :].astype(jnp.float32).reshape(pair_count, depth * plane)
    back = to_first[:, :, :plane].astype(jnp.float32).reshape(slot_count, depth * plane)
    action = jnp.dot(kept_hot, kept, precision=highest)
    action = action + jnp.dot(back_hot, back, precision=highest)
    return action.reshape(orbitals.shape)


def solution(mesh):
    return jax.shard_map(
        per_device,
        mesh=mesh,
        in_specs=(P("orb", "grp", None), P(), P()),
        out_specs=P("orb", "grp", None),
        check_vma=False,
    )
```

```python
import functools
import math

import jax
import jax.numpy as jnp
from jax import lax
from jax.experimental import pallas as pl
from jax.experimental.pallas import tpu as pltpu
from jax.sharding import PartitionSpec as P

BOX = 32
PLANE = BOX * BOX
ORB_GRP = 64
CAP = 2
SCREEN = 0.25
highest = lax.Precision.HIGHEST


def sine_table():
    counts = jnp.arange(BOX).astype(jnp.float32) + 1.0
    return jnp.sqrt(2.0 / (BOX + 1.0)) * jnp.sin(
        math.pi * counts[:, None] * counts[None, :] / (BOX + 1.0)
    )


def green_rows():
    levels = 2.0 - 2.0 * jnp.cos(
        math.pi * (jnp.arange(BOX).astype(jnp.float32) + 1.0) / (BOX + 1.0)
    )
    lanes = jnp.arange(PLANE, dtype=jnp.int32)

    def level(index):
        return 2.0 - 2.0 * jnp.cos(math.pi * (index.astype(jnp.float32) + 1.0) / (BOX + 1.0))

    return 1.0 / (levels[:, None] + (level(lanes // BOX) + level(lanes % BOX))[None, :] + SCREEN)


def halves(value):
    high = value.astype(jnp.bfloat16)
    return high, (value - high.astype(jnp.float32)).astype(jnp.bfloat16)


def dot(a, b):
    return jnp.dot(a, b, preferred_element_type=jnp.float32)


def plane_kernel(sine_ref, high_ref, low_ref):
    lane = lax.broadcasted_iota(jnp.int32, (BOX, PLANE), 1)
    row = lax.broadcasted_iota(jnp.int32, (BOX, PLANE), 0)
    by_y = jnp.where((lane >> 5) == row, 1.0, 0.0).astype(jnp.bfloat16)
    by_z = jnp.where((lane & (BOX - 1)) == row, 1.0, 0.0).astype(jnp.bfloat16)
    sine = sine_ref[...]
    parts = []
    rest = sine
    for _ in range(3):
        piece = rest.astype(jnp.bfloat16)
        parts.append(piece)
        rest = rest - piece.astype(jnp.float32)
    cols_y = dot(parts[0], by_y) + dot(parts[1], by_y) + dot(parts[2], by_y)
    cols_z = dot(parts[0], by_z) + dot(parts[1], by_z) + dot(parts[2], by_z)
    for m in range(BOX):
        block = cols_y[m : m + 1, :] * cols_z
        high = block.astype(jnp.bfloat16)
        high_ref[pl.ds(m * BOX, BOX), :] = high
        low_ref[pl.ds(m * BOX, BOX), :] = (block - high.astype(jnp.float32)).astype(jnp.bfloat16)


def plane_tables(sine):
    shape = jax.ShapeDtypeStruct((PLANE, PLANE), jnp.bfloat16)
    return pl.pallas_call(plane_kernel, out_shape=(shape, shape), name="plane_tables")(sine)


PAIR = 2


def pack_kernel(pattern, from_incoming_ref, from_own_ref, incoming_ref, orbitals_ref, out_ref):
    taken = mine = 0
    for n in range(out_ref.shape[0]):
        if pattern[n % len(pattern)]:
            out_ref[n] = incoming_ref[from_incoming_ref[taken]]
            taken += 1
        else:
            out_ref[n] = orbitals_ref[from_own_ref[mine]]
            mine += 1


def same_pair():
    row = lax.broadcasted_iota(jnp.int32, (PAIR * BOX, PAIR * BOX), 0)
    col = lax.broadcasted_iota(jnp.int32, (PAIR * BOX, PAIR * BOX), 1)
    return row, col, (row >> 5) == (col >> 5)


def steps_along_x(moves_ref, at, back):
    row, col, same = same_pair()
    step = jnp.zeros(row.shape, jnp.int32)
    for k in range(PAIR):
        step = jnp.where((row >> 5) == k, moves_ref[at + k, 0], step)
    hit = (row == col + step) if back else (col == row + step)
    return jnp.where(same & hit, 1.0, 0.0).astype(jnp.bfloat16)


def moved(value, dy, dz):
    lane = lax.broadcasted_iota(jnp.int32, value.shape, 1)
    y, z = lane >> 5, lane & (BOX - 1)
    turned = pltpu.roll(value, (PLANE - (dy * BOX + dz)) & (PLANE - 1), 1)
    inside = (y + dy >= 0) & (y + dy < BOX) & (z + dz >= 0) & (z + dz < BOX)
    return jnp.where(inside, turned, 0.0)


def solve_kernel(
    homes,
    share,
    moves_ref,
    boxes_ref,
    sine_ref,
    green_hbm,
    high_hbm,
    low_hbm,
    out_ref,
    first,
    second,
    held,
    green_ref,
    high_ref,
    low_ref,
    sems,
):
    rows = share * BOX
    depth = boxes_ref.shape[1]
    sides = BOX // depth
    copies = [
        pltpu.make_async_copy(source, into, sems.at[n])
        for n, (source, into) in enumerate(
            ((high_hbm, high_ref), (low_hbm, low_ref), (green_hbm, green_ref))
        )
    ]
    for copy in copies:
        copy.start()
    for s in range(sides):
        for k in range(share):
            at = k * BOX + s * depth
            box = s * 2 * share + k
            first[at : at + depth, :] = boxes_ref[box].astype(jnp.float32)
            second[at : at + depth, :] = boxes_ref[box + share].astype(jnp.float32)

    _, _, same = same_pair()
    wide = jnp.concatenate([jnp.concatenate([sine_ref[...]] * PAIR, 1)] * PAIR, 0)
    sine_high, sine_low = halves(jnp.where(same, wide, 0.0))
    three = jnp.concatenate([sine_high, sine_high, sine_low], 1)

    def along_x(value):
        high, low = halves(value)
        return dot(three, jnp.concatenate([high, low, high], 0))

    def along_plane(value):
        high, low = halves(value)
        both = dot(jnp.concatenate([high, low], 0), high_ref[...])
        return both[:rows] + both[rows:] + dot(high, low_ref[...])

    charges = []
    for at in range(0, share, PAIR):
        turned = [
            moved(second[k * BOX : (k + 1) * BOX, :], moves_ref[k, 1], moves_ref[k, 2])
            for k in range(at, at + PAIR)
        ]
        ahead = steps_along_x(moves_ref, at, False)
        shifted = dot(ahead, jnp.concatenate(turned, 0).astype(jnp.bfloat16))
        part = slice(at * BOX, (at + PAIR) * BOX)
        if at < homes:
            second[part, :] = shifted
        charges.append(along_x(first[part, :] * shifted))
    for copy in copies:
        copy.wait()
    modes = along_plane(jnp.concatenate(charges, 0))
    held[...] = along_plane(modes * jnp.concatenate([green_ref[...]] * share, 0))
    for at in range(0, share, PAIR):
        part = slice(at * BOX, (at + PAIR) * BOX)
        potential = along_x(held[part, :])
        if at < homes:
            held[part, :] = potential * second[part, :]
        else:
            high, low = halves(potential * first[part, :])
            back = steps_along_x(moves_ref, at, True)
            upright = dot(jnp.concatenate([back, back], 1), jnp.concatenate([high, low], 0))
            for k in range(PAIR):
                held[(at + k) * BOX : (at + k + 1) * BOX, :] = moved(
                    upright[k * BOX : (k + 1) * BOX],
                    -moves_ref[at + k, 1],
                    -moves_ref[at + k, 2],
                )
    for s in range(sides):
        for k in range(share):
            at = k * BOX + s * depth
            out_ref[s * share + k] = held[at : at + depth, :]


def take(array, index):
    return array.at[index].get(mode="promise_in_bounds")


VMEM = pl.BlockSpec(memory_space=pltpu.VMEM)
SMEM = pl.BlockSpec(memory_space=pltpu.SMEM)
HBM = pl.BlockSpec(memory_space=pltpu.HBM)
PACK_LIMIT = pltpu.CompilerParams(vmem_limit_bytes=20 << 20)
SOLVE_LIMIT = pltpu.CompilerParams(vmem_limit_bytes=61 << 20)


def packed(pattern, from_incoming, from_own, incoming, orbitals):
    shape = (from_incoming.shape[0] + from_own.shape[0], *orbitals.shape[1:])
    return pl.pallas_call(
        functools.partial(pack_kernel, pattern),
        out_shape=jax.ShapeDtypeStruct(shape, orbitals.dtype),
        in_specs=[SMEM, SMEM, VMEM, VMEM],
        out_specs=VMEM,
        compiler_params=PACK_LIMIT,
        name="pack_rows",
    )(from_incoming, from_own, incoming, orbitals)


def pair_terms(homes, boxes, moves, high, low, green, sine):
    share = moves.shape[0]
    cube = pltpu.VMEM((share * BOX, PLANE), jnp.float32)
    table = pltpu.VMEM((PLANE, PLANE), jnp.bfloat16)
    return pl.pallas_call(
        functools.partial(solve_kernel, homes, share),
        out_shape=jax.ShapeDtypeStruct((boxes.shape[0] // 2, *boxes.shape[1:]), jnp.float32),
        in_specs=[SMEM, VMEM, VMEM, HBM, HBM, HBM],
        out_specs=VMEM,
        scratch_shapes=[
            cube,
            cube,
            cube,
            pltpu.VMEM((BOX, PLANE), jnp.float32),
            table,
            table,
            pltpu.SemaphoreType.DMA((3,)),
        ],
        compiler_params=SOLVE_LIMIT,
        name="pair_terms",
    )(moves, boxes, sine, green, high, low)


def per_device(orbitals, pair_list, offsets):
    groups = lax.axis_size("orb")
    layers = lax.axis_size("grp")
    me = lax.axis_index("orb")
    region = lax.axis_index("grp")
    held, depth, plane = orbitals.shape
    slot_count = groups * CAP
    pair_count = pair_list.shape[1]
    rows_each = pair_count // layers
    slots_each = slot_count // layers
    swap = functools.partial(lax.all_to_all, split_axis=0, concat_axis=0, tiled=True)

    wanted = me * CAP + jnp.arange(CAP, dtype=jnp.int32)
    asked = pair_list[:, None, :, 2] == wanted[None, :, None]
    home_second = jnp.sum(jnp.where(asked, pair_list[:, None, :, 1], 0), axis=2)
    own = lax.dynamic_index_in_dim(pair_list, me, 0, keepdims=False)
    first_local, second_local, slot = own[:, 0], own[:, 1], own[:, 2]
    slot_ids = jnp.arange(slot_count, dtype=jnp.int32)
    named = slot[None, :] == slot_ids[:, None]
    sent_first = jnp.sum(jnp.where(named, first_local[None, :], 0), axis=1).reshape(groups, CAP)
    outgoing = jnp.concatenate([home_second, sent_first], axis=1).reshape(2 * slot_count)
    incoming = swap(take(orbitals, outgoing), "orb")

    home_second = home_second.reshape(slot_count)
    home_valid = jnp.any(asked, axis=2).reshape(slot_count)
    home_first = jnp.sum(jnp.where(asked, pair_list[:, None, :, 0], 0), axis=2).reshape(slot_count)
    from_rows = (slot // CAP * (2 * CAP) + slot % CAP).reshape(layers, rows_each)
    from_slots = (slot_ids // CAP * (2 * CAP) + CAP + slot_ids % CAP).reshape(layers, slots_each)
    pattern = (False,) * slots_each + (True,) * (rows_each + slots_each) + (False,) * rows_each
    from_incoming = jnp.concatenate([from_rows, from_slots], axis=1).reshape(-1)
    from_own = jnp.concatenate(
        [home_second.reshape(layers, slots_each), first_local.reshape(layers, rows_each)], axis=1
    ).reshape(-1)

    def part(values, count):
        return lax.dynamic_slice_in_dim(values, region * count, count, 0)

    first_ids = jnp.concatenate(
        [
            part(slot_ids // CAP * ORB_GRP + home_first, slots_each),
            part(me * ORB_GRP + first_local, rows_each),
        ]
    )
    second_ids = jnp.concatenate(
        [
            part(me * ORB_GRP + home_second, slots_each),
            part(slot // CAP * ORB_GRP + second_local, rows_each),
        ]
    )
    moves = take(offsets, first_ids) - take(offsets, second_ids)
    sine = sine_table()
    high, low = plane_tables(sine)
    green = green_rows()
    target = jnp.concatenate(
        [
            jnp.where(home_valid, home_second, held).reshape(layers, slots_each),
            first_local.reshape(layers, rows_each),
        ],
        axis=1,
    ).reshape(-1)
    hit = jnp.where(target[None, :] == jnp.arange(held, dtype=jnp.int32)[:, None], 1.0, 0.0)
    incoming, from_incoming, from_own, moves, sine, high, low, green, hit = (
        lax.optimization_barrier(
            (incoming, from_incoming, from_own, moves, sine, high, low, green, hit)
        )
    )

    boxes = swap(packed(pattern, from_incoming, from_own, incoming, orbitals), "grp")
    terms = swap(pair_terms(slots_each, boxes, moves, high, low, green, sine), "grp")
    action = jnp.dot(hit, terms.reshape(-1, depth * plane), precision=highest)
    return action.reshape(orbitals.shape)


def solution(mesh):
    return jax.shard_map(
        per_device,
        mesh=mesh,
        in_specs=(P("orb", "grp", None), P(), P()),
        out_specs=P("orb", "grp", None),
        check_vma=False,
    )
```

```python
import functools
import math

import jax
import jax.numpy as jnp
from jax import lax
from jax.experimental import pallas as pl
from jax.experimental.pallas import tpu as pltpu
from jax.sharding import PartitionSpec as P

BOX = 32
PLANE = BOX * BOX
ORB_GRP = 64
CAP = 2
SCREEN = 0.25


def sine_table():
    counts = jnp.arange(BOX).astype(jnp.float32) + 1.0
    return jnp.sqrt(2.0 / (BOX + 1.0)) * jnp.sin(
        math.pi * counts[:, None] * counts[None, :] / (BOX + 1.0)
    )


def green_rows():
    levels = 2.0 - 2.0 * jnp.cos(
        math.pi * (jnp.arange(BOX).astype(jnp.float32) + 1.0) / (BOX + 1.0)
    )
    lanes = jnp.arange(PLANE, dtype=jnp.int32)

    def level(index):
        return 2.0 - 2.0 * jnp.cos(math.pi * (index.astype(jnp.float32) + 1.0) / (BOX + 1.0))

    return 1.0 / (levels[:, None] + (level(lanes // BOX) + level(lanes % BOX))[None, :] + SCREEN)


def halves(value):
    high = value.astype(jnp.bfloat16)
    return high, (value - high.astype(jnp.float32)).astype(jnp.bfloat16)


def dot(a, b):
    return jnp.dot(a, b, preferred_element_type=jnp.float32)


TABLES = 10


def plane_kernel(sine_ref, tables_hbm, table_ref, sems):
    lane = lax.broadcasted_iota(jnp.int32, (BOX, PLANE), 1)
    row = lax.broadcasted_iota(jnp.int32, (BOX, PLANE), 0)
    by_y = jnp.where((lane >> 5) == row, 1.0, 0.0).astype(jnp.bfloat16)
    by_z = jnp.where((lane & (BOX - 1)) == row, 1.0, 0.0).astype(jnp.bfloat16)
    parts = []
    rest = sine_ref[...]
    for _ in range(3):
        piece = rest.astype(jnp.bfloat16)
        parts.append(piece)
        rest = rest - piece.astype(jnp.float32)
    cols_y = dot(parts[0], by_y) + dot(parts[1], by_y) + dot(parts[2], by_y)
    cols_z = dot(parts[0], by_z) + dot(parts[1], by_z) + dot(parts[2], by_z)
    for m in range(BOX):
        high, low = halves(cols_y[m : m + 1, :] * cols_z)
        table_ref[0, m * BOX : (m + 1) * BOX, :] = high
        table_ref[1, m * BOX : (m + 1) * BOX, :] = low
    copies = [
        pltpu.make_async_copy(table_ref.at[n], tables_hbm.at[n], sems.at[n]) for n in range(2)
    ]
    for copy in copies:
        copy.start()
    for copy in copies:
        copy.wait()


def plane_tables(sine):
    return pl.pallas_call(
        plane_kernel,
        out_shape=jax.ShapeDtypeStruct((TABLES, PLANE, PLANE), jnp.bfloat16),
        in_specs=[VMEM],
        out_specs=HBM,
        scratch_shapes=[
            pltpu.VMEM((2, PLANE, PLANE), jnp.bfloat16),
            pltpu.SemaphoreType.DMA((2,)),
        ],
        compiler_params=ROWS_LIMIT,
        name="plane_tables",
    )(sine)


PAIR = 2


def pick_kernel(sent_ref, kept_ref, orbitals_ref, sent_out, kept_out):
    for picks_ref, out_ref in ((sent_ref, sent_out), (kept_ref, kept_out)):
        for n in range(out_ref.shape[0]):
            out_ref[n] = orbitals_ref[picks_ref[n]]


def pack_kernel(pattern, picks_ref, incoming_ref, kept_ref, out_ref):
    taken = mine = 0
    for n in range(out_ref.shape[0]):
        if pattern[n % len(pattern)]:
            out_ref[n] = incoming_ref[picks_ref[taken]]
            taken += 1
        else:
            out_ref[n] = kept_ref[mine]
            mine += 1


def sum_kernel(target_ref, weight_ref, terms_ref, out_ref, *sums):
    sums = (out_ref, *sums)
    for held in sums:
        held[...] = jnp.zeros_like(held)
    for n in range(terms_ref.shape[0]):
        at = target_ref[n]
        held = sums[n % len(sums)]
        held[at] = held[at] + weight_ref[n] * terms_ref[n]
    out_ref[...] = sum(held[...] for held in sums)


def same_pair():
    row = lax.broadcasted_iota(jnp.int32, (PAIR * BOX, PAIR * BOX), 0)
    col = lax.broadcasted_iota(jnp.int32, (PAIR * BOX, PAIR * BOX), 1)
    return row, col, (row >> 5) == (col >> 5)


def steps_along_x(moves_ref, at, back):
    row, col, same = same_pair()
    step = jnp.zeros(row.shape, jnp.int32)
    for k in range(PAIR):
        step = jnp.where((row >> 5) == k, moves_ref[at + k, 0], step)
    hit = (row == col + step) if back else (col == row + step)
    return jnp.where(same & hit, 1.0, 0.0).astype(jnp.bfloat16)


def moved(value, dy, dz):
    lane = lax.broadcasted_iota(jnp.int32, value.shape, 1)
    y, z = lane >> 5, lane & (BOX - 1)
    turned = pltpu.roll(value, (PLANE - (dy * BOX + dz)) & (PLANE - 1), 1)
    inside = (y + dy >= 0) & (y + dy < BOX) & (z + dz >= 0) & (z + dz < BOX)
    return jnp.where(inside, turned, 0.0)


def solve_kernel(
    homes,
    share,
    moves_ref,
    boxes_ref,
    sine_ref,
    green_hbm,
    table_hbm,
    out_ref,
    first,
    second,
    held,
    green_ref,
    table_ref,
    sems,
):
    rows = share * BOX
    depth = boxes_ref.shape[1]
    sides = BOX // depth
    copies = [
        pltpu.make_async_copy(source, into, sems.at[n])
        for n, (source, into) in enumerate(
            ((table_hbm.at[0], table_ref.at[0]), (table_hbm.at[1], table_ref.at[1]), (green_hbm, green_ref))
        )
    ]
    for copy in copies:
        copy.start()
    for s in range(sides):
        for k in range(share):
            at = k * BOX + s * depth
            box = s * 2 * share + k
            first[at : at + depth, :] = boxes_ref[box].astype(jnp.float32)
            second[at : at + depth, :] = boxes_ref[box + share].astype(jnp.float32)

    _, _, same = same_pair()
    wide = jnp.concatenate([jnp.concatenate([sine_ref[...]] * PAIR, 1)] * PAIR, 0)
    sine_high, sine_low = halves(jnp.where(same, wide, 0.0))
    three = jnp.concatenate([sine_high, sine_high, sine_low], 1)

    def along_x(value):
        high, low = halves(value)
        return dot(three, jnp.concatenate([high, low, high], 0))

    def along_plane(value):
        high, low = halves(value)
        both = dot(jnp.concatenate([high, low], 0), table_ref[0])
        return both[:rows] + both[rows:] + dot(high, table_ref[1])

    charges = []
    for at in range(0, share, PAIR):
        turned = [
            moved(second[k * BOX : (k + 1) * BOX, :], moves_ref[k, 1], moves_ref[k, 2])
            for k in range(at, at + PAIR)
        ]
        ahead = steps_along_x(moves_ref, at, False)
        shifted = dot(ahead, jnp.concatenate(turned, 0).astype(jnp.bfloat16))
        part = slice(at * BOX, (at + PAIR) * BOX)
        if at < homes:
            second[part, :] = shifted
        charges.append(along_x(first[part, :] * shifted))
    copies[0].wait()
    high, low = halves(jnp.concatenate(charges, 0))
    both = dot(jnp.concatenate([high, low], 0), table_ref[0])
    copies[1].wait()
    modes = both[:rows] + both[rows:] + dot(high, table_ref[1])
    copies[2].wait()
    held[...] = along_plane(modes * jnp.concatenate([green_ref[...]] * share, 0))
    for at in range(0, share, PAIR):
        part = slice(at * BOX, (at + PAIR) * BOX)
        potential = along_x(held[part, :])
        if at < homes:
            held[part, :] = potential * second[part, :]
        else:
            high, low = halves(potential * first[part, :])
            back = steps_along_x(moves_ref, at, True)
            upright = dot(jnp.concatenate([back, back], 1), jnp.concatenate([high, low], 0))
            for k in range(PAIR):
                held[(at + k) * BOX : (at + k + 1) * BOX, :] = moved(
                    upright[k * BOX : (k + 1) * BOX],
                    -moves_ref[at + k, 1],
                    -moves_ref[at + k, 2],
                )
    for s in range(sides):
        for k in range(share):
            at = k * BOX + s * depth
            out_ref[s * share + k] = held[at : at + depth, :]


def take(array, index):
    return array.at[index].get(mode="promise_in_bounds")


VMEM = pl.BlockSpec(memory_space=pltpu.VMEM)
SMEM = pl.BlockSpec(memory_space=pltpu.SMEM)
HBM = pl.BlockSpec(memory_space=pltpu.HBM)
ROWS_LIMIT = pltpu.CompilerParams(vmem_limit_bytes=20 << 20)
SOLVE_LIMIT = pltpu.CompilerParams(vmem_limit_bytes=46 << 20)


def picked(sent, kept, orbitals):
    return pl.pallas_call(
        pick_kernel,
        out_shape=tuple(
            jax.ShapeDtypeStruct((n.shape[0], *orbitals.shape[1:]), orbitals.dtype)
            for n in (sent, kept)
        ),
        in_specs=[SMEM, SMEM, VMEM],
        out_specs=(VMEM, VMEM),
        compiler_params=ROWS_LIMIT,
        name="pick_rows",
    )(sent, kept, orbitals)


def summed(target, weight, terms, held):
    return pl.pallas_call(
        sum_kernel,
        out_shape=jax.ShapeDtypeStruct((held, *terms.shape[1:]), terms.dtype),
        in_specs=[SMEM, SMEM, VMEM],
        out_specs=VMEM,
        scratch_shapes=[pltpu.VMEM((held, *terms.shape[1:]), terms.dtype)] * 3,
        compiler_params=ROWS_LIMIT,
        name="sum_rows",
    )(target, weight, terms)


def packed(pattern, picks, incoming, kept):
    shape = (picks.shape[0] + kept.shape[0], *kept.shape[1:])
    return pl.pallas_call(
        functools.partial(pack_kernel, pattern),
        out_shape=jax.ShapeDtypeStruct(shape, kept.dtype),
        in_specs=[SMEM, VMEM, VMEM],
        out_specs=VMEM,
        compiler_params=ROWS_LIMIT,
        name="pack_rows",
    )(picks, incoming, kept)


def pair_terms(homes, boxes, moves, table, green, sine):
    share = moves.shape[0]
    cube = pltpu.VMEM((share * BOX, PLANE), jnp.float32)
    halves_type = pltpu.VMEM((2, PLANE, PLANE), jnp.bfloat16)
    return pl.pallas_call(
        functools.partial(solve_kernel, homes, share),
        out_shape=jax.ShapeDtypeStruct((boxes.shape[0] // 2, *boxes.shape[1:]), jnp.float32),
        in_specs=[SMEM, VMEM, VMEM, HBM, HBM],
        out_specs=VMEM,
        scratch_shapes=[
            cube,
            cube,
            cube,
            pltpu.VMEM((BOX, PLANE), jnp.float32),
            halves_type,
            pltpu.SemaphoreType.DMA((3,)),
        ],
        compiler_params=SOLVE_LIMIT,
        name="pair_terms",
    )(moves, boxes, sine, green, table)


def per_device(orbitals, pair_list, offsets):
    groups = lax.axis_size("orb")
    layers = lax.axis_size("grp")
    me = lax.axis_index("orb")
    region = lax.axis_index("grp")
    held, depth, plane = orbitals.shape
    slot_count = groups * CAP
    pair_count = pair_list.shape[1]
    rows_each = pair_count // layers
    slots_each = slot_count // layers
    swap = functools.partial(lax.all_to_all, split_axis=0, concat_axis=0, tiled=True)

    pair_list = lax.optimization_barrier(tuple(pair_list[:, :, n] for n in range(3)))
    is_me = jnp.arange(groups, dtype=jnp.int32)[:, None] == me
    first_local, second_local, slot = (
        jnp.sum(jnp.where(is_me, plane_of, 0), axis=0) for plane_of in pair_list
    )
    wanted = me * CAP + jnp.arange(CAP, dtype=jnp.int32)
    asked = pair_list[2][:, None, :] == wanted[None, :, None]
    home_second = jnp.sum(jnp.where(asked, pair_list[1][:, None, :], 0), axis=2)
    slot_ids = jnp.arange(slot_count, dtype=jnp.int32)
    named = slot[None, :] == slot_ids[:, None]
    sent_first = jnp.sum(jnp.where(named, first_local[None, :], 0), axis=1).reshape(groups, CAP)
    outgoing = jnp.concatenate([home_second, sent_first], axis=1).reshape(2 * slot_count)
    local = jnp.concatenate(
        [home_second.reshape(layers, slots_each), first_local.reshape(layers, rows_each)], axis=1
    ).reshape(-1)
    outgoing, kept = picked(outgoing, local, orbitals)
    incoming = swap(outgoing, "orb")

    home_second = home_second.reshape(slot_count)
    home_valid = jnp.any(asked, axis=2).reshape(slot_count)
    home_first = jnp.sum(jnp.where(asked, pair_list[0][:, None, :], 0), axis=2).reshape(slot_count)
    from_rows = (slot // CAP * (2 * CAP) + slot % CAP).reshape(layers, rows_each)
    from_slots = (slot_ids // CAP * (2 * CAP) + CAP + slot_ids % CAP).reshape(layers, slots_each)
    pattern = (False,) * slots_each + (True,) * (rows_each + slots_each) + (False,) * rows_each
    from_incoming = jnp.concatenate([from_rows, from_slots], axis=1).reshape(-1)

    def part(values, count):
        return lax.dynamic_slice_in_dim(values, region * count, count, 0)

    first_ids = jnp.concatenate(
        [
            part(slot_ids // CAP * ORB_GRP + home_first, slots_each),
            part(me * ORB_GRP + first_local, rows_each),
        ]
    )
    second_ids = jnp.concatenate(
        [
            part(me * ORB_GRP + home_second, slots_each),
            part(slot // CAP * ORB_GRP + second_local, rows_each),
        ]
    )
    moves = take(offsets, first_ids) - take(offsets, second_ids)
    sine = sine_table()
    table = plane_tables(sine)
    green = green_rows()
    weight = jnp.concatenate(
        [
            jnp.where(home_valid, 1.0, 0.0).reshape(layers, slots_each),
            jnp.ones((layers, rows_each), jnp.float32),
        ],
        axis=1,
    ).reshape(-1)
    incoming, from_incoming, kept, moves, sine, table, green, local, weight = (
        lax.optimization_barrier(
            (incoming, from_incoming, kept, moves, sine, table, green, local, weight)
        )
    )

    boxes = swap(packed(pattern, from_incoming, incoming, kept), "grp")
    terms = swap(pair_terms(slots_each, boxes, moves, table, green, sine), "grp")
    return summed(local, weight, terms, held)


def solution(mesh):
    return jax.shard_map(
        per_device,
        mesh=mesh,
        in_specs=(P("orb", "grp", None), P(), P()),
        out_specs=P("orb", "grp", None),
        check_vma=False,
    )
```

```python
import functools
import math

import jax
import jax.numpy as jnp
from jax import lax
from jax.experimental import pallas as pl
from jax.experimental.pallas import tpu as pltpu
from jax.sharding import PartitionSpec as P

BOX = 32
PLANE = BOX * BOX
ORB_GRP = 64
CAP = 2
SCREEN = 0.25


def sine_table():
    counts = jnp.arange(BOX).astype(jnp.float32) + 1.0
    return jnp.sqrt(2.0 / (BOX + 1.0)) * jnp.sin(
        math.pi * counts[:, None] * counts[None, :] / (BOX + 1.0)
    )


def green_rows():
    levels = 2.0 - 2.0 * jnp.cos(
        math.pi * (jnp.arange(BOX).astype(jnp.float32) + 1.0) / (BOX + 1.0)
    )
    lanes = jnp.arange(PLANE, dtype=jnp.int32)

    def level(index):
        return 2.0 - 2.0 * jnp.cos(math.pi * (index.astype(jnp.float32) + 1.0) / (BOX + 1.0))

    return 1.0 / (levels[:, None] + (level(lanes // BOX) + level(lanes % BOX))[None, :] + SCREEN)


def halves(value):
    high = value.astype(jnp.bfloat16)
    return high, (value - high.astype(jnp.float32)).astype(jnp.bfloat16)


def dot(a, b):
    return jnp.dot(a, b, preferred_element_type=jnp.float32)


TABLES = 10


def plane_kernel(sine_ref, tables_hbm, table_ref, sems):
    lane = lax.broadcasted_iota(jnp.int32, (BOX, PLANE), 1)
    row = lax.broadcasted_iota(jnp.int32, (BOX, PLANE), 0)
    by_y = jnp.where((lane >> 5) == row, 1.0, 0.0).astype(jnp.bfloat16)
    by_z = jnp.where((lane & (BOX - 1)) == row, 1.0, 0.0).astype(jnp.bfloat16)
    parts = []
    rest = sine_ref[...]
    for _ in range(3):
        piece = rest.astype(jnp.bfloat16)
        parts.append(piece)
        rest = rest - piece.astype(jnp.float32)
    cols_y = dot(parts[0], by_y) + dot(parts[1], by_y) + dot(parts[2], by_y)
    cols_z = dot(parts[0], by_z) + dot(parts[1], by_z) + dot(parts[2], by_z)
    for m in range(BOX):
        high, low = halves(cols_y[m : m + 1, :] * cols_z)
        table_ref[0, m * BOX : (m + 1) * BOX, :] = high
        table_ref[1, m * BOX : (m + 1) * BOX, :] = low
    copies = [
        pltpu.make_async_copy(table_ref.at[n], tables_hbm.at[n], sems.at[n]) for n in range(2)
    ]
    for copy in copies:
        copy.start()
    for copy in copies:
        copy.wait()


def plane_tables(sine):
    return pl.pallas_call(
        plane_kernel,
        out_shape=jax.ShapeDtypeStruct((TABLES, PLANE, PLANE), jnp.bfloat16),
        in_specs=[VMEM],
        out_specs=HBM,
        scratch_shapes=[
            pltpu.VMEM((2, PLANE, PLANE), jnp.bfloat16),
            pltpu.SemaphoreType.DMA((2,)),
        ],
        compiler_params=SOLVE_LIMIT,
        name="plane_tables",
    )(sine)


SIDE = 4
PAIR = 2


def pick_kernel(each, place_ref, sent_ref, local_ref, orbitals_ref, sent_out, *local_outs):
    for n in range(sent_out.shape[0]):
        sent_out[n] = orbitals_ref[sent_ref[n]]
    for step, out_ref in enumerate(local_outs):
        side = (place_ref[1] + step) & (SIDE - 1)
        for other in range(SIDE):
            for q in range(each):
                pick = local_ref[(other * SIDE + side) * each + q]
                out_ref[other * each + q] = orbitals_ref[pick]


def turn_kernel(each, place_ref, *refs):
    came, gone = refs[:SIDE], refs[SIDE:]
    for step, out_ref in enumerate(gone):
        other = (place_ref[0] + step) & (SIDE - 1)
        for n, in_ref in enumerate(came):
            for q in range(each):
                out_ref[n * each + q] = in_ref[other * each + q]


def settle_kernel(each, place_ref, *refs):
    came, out_ref = refs[:SIDE], refs[SIDE]
    for far, in_ref in enumerate(came):
        y = (place_ref[0] - far) & (SIDE - 1)
        for near in range(SIDE):
            side = y * SIDE + ((place_ref[1] - near) & (SIDE - 1))
            for q in range(each):
                out_ref[side * each + q] = in_ref[near * each + q]


def pack_kernel(picks_ref, incoming_ref, out_ref):
    for n in range(out_ref.shape[0]):
        out_ref[n] = incoming_ref[picks_ref[n]]


def sum_kernel(target_ref, weight_ref, terms_ref, out_ref, *sums):
    sums = (out_ref, *sums)
    for held in sums:
        held[...] = jnp.zeros_like(held)
    for n in range(terms_ref.shape[0]):
        at = target_ref[n]
        held = sums[n % len(sums)]
        held[at] = held[at] + weight_ref[n] * terms_ref[n]
    out_ref[...] = sum(held[...] for held in sums)


def same_pair():
    row = lax.broadcasted_iota(jnp.int32, (PAIR * BOX, PAIR * BOX), 0)
    col = lax.broadcasted_iota(jnp.int32, (PAIR * BOX, PAIR * BOX), 1)
    return row, col, (row >> 5) == (col >> 5)


def steps_along_x(moves_ref, at, back):
    row, col, same = same_pair()
    step = jnp.zeros(row.shape, jnp.int32)
    for k in range(PAIR):
        step = jnp.where((row >> 5) == k, moves_ref[3 * (at + k)], step)
    hit = (row == col + step) if back else (col == row + step)
    return jnp.where(same & hit, 1.0, 0.0).astype(jnp.bfloat16)


def moved(value, dy, dz):
    lane = lax.broadcasted_iota(jnp.int32, value.shape, 1)
    y, z = lane >> 5, lane & (BOX - 1)
    turned = pltpu.roll(value, (PLANE - (dy * BOX + dz)) & (PLANE - 1), 1)
    inside = (y + dy >= 0) & (y + dy < BOX) & (z + dz >= 0) & (z + dz < BOX)
    return jnp.where(inside, turned, 0.0)


def solve_kernel(
    homes,
    share,
    moves_ref,
    boxes_ref,
    local_ref,
    sine_ref,
    green_hbm,
    table_hbm,
    out_ref,
    first,
    second,
    held,
    green_ref,
    table_ref,
    sems,
):
    rows = share * BOX
    depth = boxes_ref.shape[1]
    sides = BOX // depth
    copies = [
        pltpu.make_async_copy(source, into, sems.at[n])
        for n, (source, into) in enumerate(
            ((table_hbm.at[0], table_ref.at[0]), (table_hbm.at[1], table_ref.at[1]), (green_hbm, green_ref))
        )
    ]
    for copy in copies:
        copy.start()
    for s in range(sides):
        for k in range(share):
            at = k * BOX + s * depth
            mine = second if k < homes else first
            q = s * share + (share - homes + k if k < homes else k - homes)
            mine[at : at + depth, :] = boxes_ref[q].astype(jnp.float32)
            other = first if k < homes else second
            other[at : at + depth, :] = local_ref[s * share + k].astype(jnp.float32)

    _, _, same = same_pair()
    wide = jnp.concatenate([jnp.concatenate([sine_ref[...]] * PAIR, 1)] * PAIR, 0)
    sine_high, sine_low = halves(jnp.where(same, wide, 0.0))
    three = jnp.concatenate([sine_high, sine_high, sine_low], 1)

    def along_x(value):
        high, low = halves(value)
        return dot(three, jnp.concatenate([high, low, high], 0))

    def along_plane(value):
        high, low = halves(value)
        both = dot(jnp.concatenate([high, low], 0), table_ref[0])
        return both[:rows] + both[rows:] + dot(high, table_ref[1])

    charges = []
    for at in range(0, share, PAIR):
        turned = [
            moved(second[k * BOX : (k + 1) * BOX, :], moves_ref[3 * k + 1], moves_ref[3 * k + 2])
            for k in range(at, at + PAIR)
        ]
        ahead = steps_along_x(moves_ref, at, False)
        shifted = dot(ahead, jnp.concatenate(turned, 0).astype(jnp.bfloat16))
        part = slice(at * BOX, (at + PAIR) * BOX)
        if at < homes:
            second[part, :] = shifted
        charges.append(along_x(first[part, :] * shifted))
    copies[0].wait()
    high, low = halves(jnp.concatenate(charges, 0))
    both = dot(jnp.concatenate([high, low], 0), table_ref[0])
    copies[1].wait()
    modes = both[:rows] + both[rows:] + dot(high, table_ref[1])
    copies[2].wait()
    held[...] = along_plane(modes * jnp.concatenate([green_ref[...]] * share, 0))
    for at in range(0, share, PAIR):
        part = slice(at * BOX, (at + PAIR) * BOX)
        potential = along_x(held[part, :])
        if at < homes:
            held[part, :] = potential * second[part, :]
        else:
            high, low = halves(potential * first[part, :])
            back = steps_along_x(moves_ref, at, True)
            upright = dot(jnp.concatenate([back, back], 1), jnp.concatenate([high, low], 0))
            for k in range(PAIR):
                held[(at + k) * BOX : (at + k + 1) * BOX, :] = moved(
                    upright[k * BOX : (k + 1) * BOX],
                    -moves_ref[3 * (at + k) + 1],
                    -moves_ref[3 * (at + k) + 2],
                )
    for s in range(sides):
        for k in range(share):
            at = k * BOX + s * depth
            out_ref[s * share + k] = held[at : at + depth, :]


VMEM = pl.BlockSpec(memory_space=pltpu.VMEM)
SMEM = pl.BlockSpec(memory_space=pltpu.SMEM)
HBM = pl.BlockSpec(memory_space=pltpu.HBM)
ROWS_LIMIT = pltpu.CompilerParams(vmem_limit_bytes=20 << 20)
SOLVE_LIMIT = pltpu.CompilerParams(vmem_limit_bytes=46 << 20)


def rows_call(kernel, name, counts, in_specs, box, *args):
    out = tuple(jax.ShapeDtypeStruct((n, *box.shape[1:]), box.dtype) for n in counts)
    return pl.pallas_call(
        kernel,
        out_shape=out,
        in_specs=in_specs,
        out_specs=(VMEM,) * len(out),
        compiler_params=ROWS_LIMIT,
        name=name,
    )(*args)


def along(array, step, axis):
    pairs = []
    for n in range(SIDE * SIDE):
        at = list(divmod(n, SIDE))
        at[axis] = (at[axis] + step) % SIDE
        pairs.append((n, at[0] * SIDE + at[1]))
    return lax.ppermute(array, "grp", pairs)


def summed(target, weight, terms, held):
    return pl.pallas_call(
        sum_kernel,
        out_shape=jax.ShapeDtypeStruct((held, *terms.shape[1:]), terms.dtype),
        in_specs=[SMEM, SMEM, VMEM],
        out_specs=VMEM,
        scratch_shapes=[pltpu.VMEM((held, *terms.shape[1:]), terms.dtype)] * 3,
        compiler_params=ROWS_LIMIT,
        name="sum_rows",
    )(target, weight, terms)


def pair_terms(homes, boxes, local, moves, table, green, sine):
    share = moves.shape[0] // 3
    cube = pltpu.VMEM((share * BOX, PLANE), jnp.float32)
    halves_type = pltpu.VMEM((2, PLANE, PLANE), jnp.bfloat16)
    return pl.pallas_call(
        functools.partial(solve_kernel, homes, share),
        out_shape=jax.ShapeDtypeStruct(boxes.shape, jnp.float32),
        in_specs=[SMEM, VMEM, VMEM, VMEM, HBM, HBM],
        out_specs=VMEM,
        scratch_shapes=[
            cube,
            cube,
            cube,
            pltpu.VMEM((BOX, PLANE), jnp.float32),
            halves_type,
            pltpu.SemaphoreType.DMA((3,)),
        ],
        compiler_params=SOLVE_LIMIT,
        name="pair_terms",
    )(moves, boxes, local, sine, green, table)


def per_device(orbitals, pair_list, offsets):
    groups = lax.axis_size("orb")
    layers = lax.axis_size("grp")
    me = lax.axis_index("orb")
    region = lax.axis_index("grp")
    held, depth, plane = orbitals.shape
    slot_count = groups * CAP
    pair_count = pair_list.shape[1]
    rows_each = pair_count // layers
    slots_each = slot_count // layers
    swap = functools.partial(lax.all_to_all, split_axis=0, concat_axis=0, tiled=True)

    pair_list = lax.optimization_barrier(tuple(pair_list[:, :, n] for n in range(3)))
    is_me = jnp.arange(groups, dtype=jnp.int32)[:, None] == me
    first_local, second_local, slot = (
        jnp.sum(jnp.where(is_me, plane_of, 0), axis=0) for plane_of in pair_list
    )
    wanted = me * CAP + jnp.arange(CAP, dtype=jnp.int32)
    asked = pair_list[2][:, None, :] == wanted[None, :, None]
    home_second = jnp.sum(jnp.where(asked, pair_list[1][:, None, :], 0), axis=2)
    slot_ids = jnp.arange(slot_count, dtype=jnp.int32)
    named = slot[None, :] == slot_ids[:, None]
    sent_first = jnp.sum(jnp.where(named, first_local[None, :], 0), axis=1).reshape(groups, CAP)
    outgoing = jnp.concatenate([home_second, sent_first], axis=1).reshape(2 * slot_count)
    local = jnp.concatenate(
        [home_second.reshape(layers, slots_each), first_local.reshape(layers, rows_each)], axis=1
    ).reshape(-1)
    each = rows_each + slots_each
    side_rows = SIDE * each
    place = jnp.stack([region // SIDE, region % SIDE])
    outgoing, *local_rows = rows_call(
        functools.partial(pick_kernel, each),
        "pick_rows",
        (2 * slot_count,) + (side_rows,) * SIDE,
        [SMEM, SMEM, SMEM, VMEM],
        orbitals,
        place,
        outgoing,
        local,
        orbitals,
    )
    incoming = swap(outgoing, "orb")

    came = [local_rows[0]] + [along(local_rows[n], n, 1) for n in range(1, SIDE)]
    turned = rows_call(
        functools.partial(turn_kernel, each),
        "turn_rows",
        (side_rows,) * SIDE,
        [SMEM] + [VMEM] * SIDE,
        orbitals,
        place,
        *came,
    )
    (whole,) = rows_call(
        functools.partial(settle_kernel, each),
        "settle_rows",
        (layers * each,),
        [SMEM] + [VMEM] * SIDE,
        orbitals,
        place,
        turned[0],
        *(along(turned[n], n, 0) for n in range(1, SIDE)),
    )

    home_second = home_second.reshape(slot_count)
    home_valid = jnp.any(asked, axis=2).reshape(slot_count)
    home_first = jnp.sum(jnp.where(asked, pair_list[0][:, None, :], 0), axis=2).reshape(slot_count)
    from_rows = (slot // CAP * (2 * CAP) + slot % CAP).reshape(layers, rows_each)
    from_slots = (slot_ids // CAP * (2 * CAP) + CAP + slot_ids % CAP).reshape(layers, slots_each)
    from_incoming = jnp.concatenate([from_rows, from_slots], axis=1).reshape(-1)

    def part(values, count):
        return lax.dynamic_slice_in_dim(values, region * count, count, 0)

    first_ids = jnp.concatenate(
        [
            part(slot_ids // CAP * ORB_GRP + home_first, slots_each),
            part(me * ORB_GRP + first_local, rows_each),
        ]
    )
    second_ids = jnp.concatenate(
        [
            part(me * ORB_GRP + home_second, slots_each),
            part(slot // CAP * ORB_GRP + second_local, rows_each),
        ]
    )
    ids = jnp.arange(offsets.shape[0], dtype=jnp.int32)
    signs = (first_ids[:, None] == ids).astype(jnp.int32) - (
        second_ids[:, None] == ids
    ).astype(jnp.int32)
    moves = jnp.sum(signs[:, None, :] * offsets.T[None, :, :], axis=2).reshape(-1)
    sine = sine_table()
    table = plane_tables(sine)
    green = green_rows()
    weight = jnp.concatenate(
        [
            jnp.where(home_valid, 1.0, 0.0).reshape(layers, slots_each),
            jnp.ones((layers, rows_each), jnp.float32),
        ],
        axis=1,
    ).reshape(-1)
    incoming, from_incoming, whole, moves, sine, table, green, local, weight = (
        lax.optimization_barrier(
            (incoming, from_incoming, whole, moves, sine, table, green, local, weight)
        )
    )

    (boxes,) = rows_call(
        pack_kernel,
        "pack_rows",
        (layers * each,),
        [SMEM, VMEM],
        orbitals,
        from_incoming,
        incoming,
    )
    boxes = swap(boxes, "grp")
    terms = pair_terms(slots_each, boxes, whole, moves, table, green, sine)
    terms = swap(terms, "grp")
    return summed(local, weight, terms, held)


def solution(mesh):
    return jax.shard_map(
        per_device,
        mesh=mesh,
        in_specs=(P("orb", "grp", None), P(), P()),
        out_specs=P("orb", "grp", None),
        check_vma=False,
    )
```

```python
import functools
import math

import jax
import jax.numpy as jnp
from jax import lax
from jax.experimental import pallas as pl
from jax.experimental.pallas import tpu as pltpu
from jax.sharding import PartitionSpec as P

BOX = 32
PLANE = BOX * BOX
HALF = PLANE // 2
LANES = 128
ORB_GRP = 64
CAP = 2
SCREEN = 0.25


def sine_table():
    counts = jnp.arange(BOX).astype(jnp.float32) + 1.0
    return jnp.sqrt(2.0 / (BOX + 1.0)) * jnp.sin(
        math.pi * counts[:, None] * counts[None, :] / (BOX + 1.0)
    )


def plane_modes(lanes):
    odd, place = lanes >> 9, lanes & (HALF - 1)
    y = place >> 4
    return y, 2 * (place & 15) + ((y + odd) & 1)


def green_rows():
    def level(index):
        return 2.0 - 2.0 * jnp.cos(math.pi * (index.astype(jnp.float32) + 1.0) / (BOX + 1.0))

    y, z = plane_modes(jnp.arange(PLANE, dtype=jnp.int32))
    x = level(jnp.arange(BOX, dtype=jnp.int32))
    return 1.0 / (x[:, None] + (level(y) + level(z))[None, :] + SCREEN)


def halves(value):
    high = value.astype(jnp.bfloat16)
    return high, (value - high.astype(jnp.float32)).astype(jnp.bfloat16)


def dot(a, b):
    return jnp.dot(a, b, preferred_element_type=jnp.float32)


def dot_back(a, b):
    return lax.dot_general(a, b, (((1,), (1,)), ((), ())), preferred_element_type=jnp.float32)


TABLES = 40


def plane_kernel(sine_ref, tables_hbm, table_ref, sems):
    lane = lax.broadcasted_iota(jnp.int32, (BOX, PLANE), 1)
    row = lax.broadcasted_iota(jnp.int32, (BOX, PLANE), 0)
    y, z = plane_modes(lane)
    by_y = jnp.where(y == row, 1.0, 0.0).astype(jnp.bfloat16)
    by_z = jnp.where(z == row, 1.0, 0.0).astype(jnp.bfloat16)
    parts = []
    rest = sine_ref[...]
    for _ in range(3):
        piece = rest.astype(jnp.bfloat16)
        parts.append(piece)
        rest = rest - piece.astype(jnp.float32)
    cols_y = dot(parts[0], by_y) + dot(parts[1], by_y) + dot(parts[2], by_y)
    cols_z = dot(parts[0], by_z) + dot(parts[1], by_z) + dot(parts[2], by_z)
    for m in range(BOX // 2):
        high, low = halves(cols_y[m : m + 1, :] * cols_z)
        part = slice(m * BOX, (m + 1) * BOX)
        for odd in range(2):
            modes = slice(odd * HALF, (odd + 1) * HALF)
            table_ref[2 * odd, part, :] = high[:, modes]
            table_ref[2 * odd + 1, part, :] = low[:, modes]
    copies = [
        pltpu.make_async_copy(table_ref.at[n], tables_hbm.at[n], sems.at[n]) for n in range(4)
    ]
    for copy in copies:
        copy.start()
    for copy in copies:
        copy.wait()


def plane_tables(sine):
    return pl.pallas_call(
        plane_kernel,
        out_shape=jax.ShapeDtypeStruct((TABLES, HALF, HALF), jnp.bfloat16),
        in_specs=[VMEM],
        out_specs=HBM,
        scratch_shapes=[
            pltpu.VMEM((4, HALF, HALF), jnp.bfloat16),
            pltpu.SemaphoreType.DMA((4,)),
        ],
        compiler_params=SOLVE_LIMIT,
        name="plane_tables",
    )(sine)


SIDE = 4
PAIR = 2


def pick_kernel(lists_ref, orbitals_ref, sent_out, *refs):
    local_outs, (columns, rows, picks_ref, own_ref, sems) = refs[:SIDE], refs[SIDE:]
    groups, pair_count = lists_ref.shape[1:]
    slots_each, rows_each = groups * CAP // SIDE**2, pair_count // SIDE**2
    each = slots_each + rows_each
    me = lax.axis_index("orb")
    x = lax.axis_index("grp") & (SIDE - 1)
    second = lists_ref[1].astype(jnp.float32)
    own_first = lists_ref[0, pl.ds(me, 1), :].astype(jnp.float32)
    own_slot = lists_ref[2, pl.ds(me, 1), :]
    group = lax.broadcasted_iota(jnp.int32, (groups, pair_count), 0)
    lane = lax.broadcasted_iota(jnp.int32, (groups, LANES), 1)
    table = jnp.zeros((groups, LANES), jnp.float32)
    for c in range(CAP):
        asked = jnp.where(lists_ref[2] == me * CAP + c, second, 0.0)
        named = jnp.where(own_slot == group * CAP + c, own_first, 0.0)
        table = jnp.where(lane == c, jnp.sum(asked, axis=1, keepdims=True), table)
        table = jnp.where(lane == CAP + c, jnp.sum(named, axis=1, keepdims=True), table)
    columns[...] = table.astype(jnp.int32)
    rows[...] = jnp.zeros_like(rows)
    rows[0:1, 0:pair_count] = own_first.astype(jnp.int32)
    copies = [
        pltpu.make_async_copy(columns, picks_ref, sems.at[0]),
        pltpu.make_async_copy(rows, own_ref, sems.at[1]),
    ]
    for copy in copies:
        copy.start()
    for copy in copies:
        copy.wait()
    for n in range(groups):
        for c in range(2 * CAP):
            sent_out[n * 2 * CAP + c] = orbitals_ref[picks_ref[n, c]]
    for step, out_ref in enumerate(local_outs):
        for y in range(SIDE):
            side = y * SIDE + ((x + step) & (SIDE - 1))
            for q in range(slots_each):
                pick = picks_ref[side * (slots_each // CAP) + q // CAP, q % CAP]
                out_ref[y * each + q] = orbitals_ref[pick]
            for q in range(rows_each):
                pick = own_ref[0, side * rows_each + q]
                out_ref[y * each + slots_each + q] = orbitals_ref[pick]


def turn_kernel(each, place_ref, *refs):
    came, gone = refs[:SIDE], refs[SIDE:]
    for step, out_ref in enumerate(gone):
        other = (place_ref[0] + step) & (SIDE - 1)
        for n, in_ref in enumerate(came):
            for q in range(each):
                out_ref[n * each + q] = in_ref[other * each + q]


def settle_kernel(each, place_ref, *refs):
    came, out_ref = refs[:SIDE], refs[SIDE]
    for far, in_ref in enumerate(came):
        y = (place_ref[0] - far) & (SIDE - 1)
        for near in range(SIDE):
            side = y * SIDE + ((place_ref[1] - near) & (SIDE - 1))
            for q in range(each):
                out_ref[side * each + q] = in_ref[near * each + q]


def pack_kernel(picks_ref, incoming_ref, out_ref):
    for n in range(out_ref.shape[0]):
        out_ref[n] = incoming_ref[picks_ref[n]]


def sum_kernel(target_ref, weight_ref, terms_ref, out_ref, *sums):
    sums = (out_ref, *sums)
    for held in sums:
        held[...] = jnp.zeros_like(held)
    for n in range(terms_ref.shape[0]):
        at = target_ref[n]
        held = sums[n % len(sums)]
        held[at] = held[at] + weight_ref[n] * terms_ref[n]
    out_ref[...] = sum(held[...] for held in sums)


def same_pair():
    row = lax.broadcasted_iota(jnp.int32, (PAIR * BOX, PAIR * BOX), 0)
    col = lax.broadcasted_iota(jnp.int32, (PAIR * BOX, PAIR * BOX), 1)
    return row, col, (row >> 5) == (col >> 5)


def steps_along_x(moves_ref, at, back):
    row, col, same = same_pair()
    step = jnp.zeros(row.shape, jnp.int32)
    for k in range(PAIR):
        step = jnp.where((row >> 5) == k, moves_ref[3 * (at + k)], step)
    hit = (row == col + step) if back else (col == row + step)
    return jnp.where(same & hit, 1.0, 0.0).astype(jnp.bfloat16)


def moved(value, dy, dz):
    lane = lax.broadcasted_iota(jnp.int32, value.shape, 1)
    y, z = lane >> 5, lane & (BOX - 1)
    turned = pltpu.roll(value, (PLANE - (dy * BOX + dz)) & (PLANE - 1), 1)
    inside = (y + dy >= 0) & (y + dy < BOX) & (z + dz >= 0) & (z + dz < BOX)
    return jnp.where(inside, turned, 0.0)


def solve_kernel(
    homes,
    share,
    moves_ref,
    boxes_ref,
    local_ref,
    sine_ref,
    green_hbm,
    table_hbm,
    out_ref,
    first,
    second,
    held,
    green_ref,
    table_ref,
    sems,
):
    rows = share * BOX
    depth = boxes_ref.shape[1]
    sides = BOX // depth
    copies = [
        pltpu.make_async_copy(table_hbm.at[n], table_ref.at[n], sems.at[n]) for n in range(4)
    ] + [pltpu.make_async_copy(green_hbm, green_ref, sems.at[4])]
    for copy in copies:
        copy.start()
    for s in range(sides):
        for k in range(share):
            at = k * BOX + s * depth
            mine = second if k < homes else first
            q = s * share + (share - homes + k if k < homes else k - homes)
            mine[at : at + depth, :] = boxes_ref[q].astype(jnp.float32)
            other = first if k < homes else second
            other[at : at + depth, :] = local_ref[s * share + k].astype(jnp.float32)

    _, _, same = same_pair()
    wide = jnp.concatenate([jnp.concatenate([sine_ref[...]] * PAIR, 1)] * PAIR, 0)
    sine_high, sine_low = halves(jnp.where(same, wide, 0.0))
    three = jnp.concatenate([sine_high, sine_high, sine_low], 1)

    def along_x(value):
        high, low = halves(value)
        return dot(three, jnp.concatenate([high, low, high], 0))

    def mirrored(value):
        back = LANES - 1 - lax.broadcasted_iota(jnp.int32, (value.shape[0], LANES), 1)
        blocks = [value[:, n : n + LANES] for n in range(0, HALF, LANES)]
        return jnp.concatenate(
            [jnp.take_along_axis(block, back, axis=1) for block in reversed(blocks)], 1
        )

    def to_modes(value):
        near, far = value[:, :HALF], mirrored(value[:, HALF:])
        modes = []
        for n, part in ((0, near + far), (2, near - far)):
            high, low = halves(part)
            copies[n].wait()
            both = dot(jnp.concatenate([high, low], 0), table_ref[n])
            copies[n + 1].wait()
            modes.append(both[:rows] + both[rows:] + dot(high, table_ref[n + 1]))
        return jnp.concatenate(modes, 1)

    def to_cells(modes):
        even, odd = [], []
        for n, part, into in ((0, modes[:, :HALF], even), (2, modes[:, HALF:], odd)):
            high, low = halves(part)
            both = dot_back(jnp.concatenate([high, low], 0), table_ref[n])
            into.append(both[:rows] + both[rows:] + dot_back(high, table_ref[n + 1]))
        return jnp.concatenate([even[0] + odd[0], mirrored(even[0] - odd[0])], 1)

    charges = []
    for at in range(0, share, PAIR):
        turned = [
            moved(second[k * BOX : (k + 1) * BOX, :], moves_ref[3 * k + 1], moves_ref[3 * k + 2])
            for k in range(at, at + PAIR)
        ]
        ahead = steps_along_x(moves_ref, at, False)
        shifted = dot(ahead, jnp.concatenate(turned, 0).astype(jnp.bfloat16))
        part = slice(at * BOX, (at + PAIR) * BOX)
        if at < homes:
            second[part, :] = shifted
        charges.append(along_x(first[part, :] * shifted))
    modes = to_modes(jnp.concatenate(charges, 0))
    copies[4].wait()
    held[...] = to_cells(modes * jnp.concatenate([green_ref[...]] * share, 0))
    for at in range(0, share, PAIR):
        part = slice(at * BOX, (at + PAIR) * BOX)
        potential = along_x(held[part, :])
        if at < homes:
            held[part, :] = potential * second[part, :]
        else:
            high, low = halves(potential * first[part, :])
            back = steps_along_x(moves_ref, at, True)
            upright = dot(jnp.concatenate([back, back], 1), jnp.concatenate([high, low], 0))
            for k in range(PAIR):
                held[(at + k) * BOX : (at + k + 1) * BOX, :] = moved(
                    upright[k * BOX : (k + 1) * BOX],
                    -moves_ref[3 * (at + k) + 1],
                    -moves_ref[3 * (at + k) + 2],
                )
    for s in range(sides):
        for k in range(share):
            at = k * BOX + s * depth
            out_ref[s * share + k] = held[at : at + depth, :]


VMEM = pl.BlockSpec(memory_space=pltpu.VMEM)
SMEM = pl.BlockSpec(memory_space=pltpu.SMEM)
HBM = pl.BlockSpec(memory_space=pltpu.HBM)
ROWS_LIMIT = pltpu.CompilerParams(vmem_limit_bytes=20 << 20)
PICK_LIMIT = pltpu.CompilerParams(vmem_limit_bytes=66_900_000)
SOLVE_LIMIT = pltpu.CompilerParams(vmem_limit_bytes=46 << 20)


def rows_call(kernel, name, counts, in_specs, box, *args, scratch=(), limit=ROWS_LIMIT):
    out = tuple(jax.ShapeDtypeStruct((n, *box.shape[1:]), box.dtype) for n in counts)
    return pl.pallas_call(
        kernel,
        out_shape=out,
        in_specs=in_specs,
        out_specs=(VMEM,) * len(out),
        scratch_shapes=scratch,
        compiler_params=limit,
        name=name,
    )(*args)


def along(array, step, axis):
    pairs = []
    for n in range(SIDE * SIDE):
        at = list(divmod(n, SIDE))
        at[axis] = (at[axis] + step) % SIDE
        pairs.append((n, at[0] * SIDE + at[1]))
    return lax.ppermute(array, "grp", pairs)


def summed(target, weight, terms, held):
    return pl.pallas_call(
        sum_kernel,
        out_shape=jax.ShapeDtypeStruct((held, *terms.shape[1:]), terms.dtype),
        in_specs=[SMEM, SMEM, VMEM],
        out_specs=VMEM,
        scratch_shapes=[pltpu.VMEM((held, *terms.shape[1:]), terms.dtype)] * 3,
        compiler_params=ROWS_LIMIT,
        name="sum_rows",
    )(target, weight, terms)


def pair_terms(homes, boxes, local, moves, table, green, sine):
    share = moves.shape[0] // 3
    cube = pltpu.VMEM((share * BOX, PLANE), jnp.float32)
    halves_type = pltpu.VMEM((4, HALF, HALF), jnp.bfloat16)
    return pl.pallas_call(
        functools.partial(solve_kernel, homes, share),
        out_shape=jax.ShapeDtypeStruct(boxes.shape, jnp.float32),
        in_specs=[SMEM, VMEM, VMEM, VMEM, HBM, HBM],
        out_specs=VMEM,
        scratch_shapes=[
            cube,
            cube,
            cube,
            pltpu.VMEM((BOX, PLANE), jnp.float32),
            halves_type,
            pltpu.SemaphoreType.DMA((5,)),
        ],
        compiler_params=SOLVE_LIMIT,
        name="pair_terms",
    )(moves, boxes, local, sine, green, table)


def per_device(orbitals, pair_list, offsets):
    groups = lax.axis_size("orb")
    layers = lax.axis_size("grp")
    me = lax.axis_index("orb")
    region = lax.axis_index("grp")
    held, depth, plane = orbitals.shape
    slot_count = groups * CAP
    pair_count = pair_list.shape[1]
    rows_each = pair_count // layers
    slots_each = slot_count // layers
    swap = functools.partial(lax.all_to_all, split_axis=0, concat_axis=0, tiled=True)

    each = rows_each + slots_each
    side_rows = SIDE * each
    lists = jnp.transpose(pair_list, (2, 0, 1))
    outgoing, *local_rows = rows_call(
        pick_kernel,
        "pick_rows",
        (2 * slot_count,) + (side_rows,) * SIDE,
        [VMEM, VMEM],
        orbitals,
        lists,
        orbitals,
        scratch=[
            pltpu.VMEM((groups, LANES), jnp.int32),
            pltpu.VMEM((8, LANES), jnp.int32),
            pltpu.SMEM((groups, LANES), jnp.int32),
            pltpu.SMEM((8, LANES), jnp.int32),
            pltpu.SemaphoreType.DMA((2,)),
        ],
        limit=PICK_LIMIT,
    )
    incoming = swap(outgoing, "orb")

    place = jnp.stack([region // SIDE, region % SIDE])
    came = [local_rows[0]] + [along(local_rows[n], n, 1) for n in range(1, SIDE)]
    turned = rows_call(
        functools.partial(turn_kernel, each),
        "turn_rows",
        (side_rows,) * SIDE,
        [SMEM] + [VMEM] * SIDE,
        orbitals,
        place,
        *came,
    )
    (whole,) = rows_call(
        functools.partial(settle_kernel, each),
        "settle_rows",
        (layers * each,),
        [SMEM] + [VMEM] * SIDE,
        orbitals,
        place,
        turned[0],
        *(along(turned[n], n, 0) for n in range(1, SIDE)),
    )

    first_of, second_of, slot_of = lax.optimization_barrier(tuple(lists[n] for n in range(3)))
    is_me = jnp.arange(groups, dtype=jnp.int32)[:, None] == me
    first_local, second_local, slot = (
        jnp.sum(jnp.where(is_me, values, 0), axis=0) for values in (first_of, second_of, slot_of)
    )
    slot_ids = jnp.arange(slot_count, dtype=jnp.int32)
    wanted = me * CAP + jnp.arange(CAP, dtype=jnp.int32)
    asked = slot_of[:, None, :] == wanted[None, :, None]
    home_second = jnp.sum(jnp.where(asked, second_of[:, None, :], 0), axis=2).reshape(slot_count)
    local = jnp.concatenate(
        [home_second.reshape(layers, slots_each), first_local.reshape(layers, rows_each)], axis=1
    ).reshape(-1)
    home_valid = jnp.any(asked, axis=2).reshape(slot_count)
    home_first = jnp.sum(jnp.where(asked, first_of[:, None, :], 0), axis=2).reshape(slot_count)
    from_rows = (slot // CAP * (2 * CAP) + slot % CAP).reshape(layers, rows_each)
    from_slots = (slot_ids // CAP * (2 * CAP) + CAP + slot_ids % CAP).reshape(layers, slots_each)
    from_incoming = jnp.concatenate([from_rows, from_slots], axis=1).reshape(-1)

    def part(values, count):
        return lax.dynamic_slice_in_dim(values, region * count, count, 0)

    first_ids = jnp.concatenate(
        [
            part(slot_ids // CAP * ORB_GRP + home_first, slots_each),
            part(me * ORB_GRP + first_local, rows_each),
        ]
    )
    second_ids = jnp.concatenate(
        [
            part(me * ORB_GRP + home_second, slots_each),
            part(slot // CAP * ORB_GRP + second_local, rows_each),
        ]
    )
    ids = jnp.arange(offsets.shape[0], dtype=jnp.int32)
    signs = (first_ids[:, None] == ids).astype(jnp.int32) - (
        second_ids[:, None] == ids
    ).astype(jnp.int32)
    moves = jnp.sum(signs[:, None, :] * offsets.T[None, :, :], axis=2).reshape(-1)
    sine = sine_table()
    table = plane_tables(sine)
    green = green_rows()
    weight = jnp.concatenate(
        [
            jnp.where(home_valid, 1.0, 0.0).reshape(layers, slots_each),
            jnp.ones((layers, rows_each), jnp.float32),
        ],
        axis=1,
    ).reshape(-1)
    incoming, from_incoming, whole, moves, sine, table, green, local, weight = (
        lax.optimization_barrier(
            (incoming, from_incoming, whole, moves, sine, table, green, local, weight)
        )
    )

    (boxes,) = rows_call(
        pack_kernel,
        "pack_rows",
        (layers * each,),
        [SMEM, VMEM],
        orbitals,
        from_incoming,
        incoming,
    )
    boxes = swap(boxes, "grp")
    terms = pair_terms(slots_each, boxes, whole, moves, table, green, sine)
    terms = swap(terms, "grp")
    return summed(local, weight, terms, held)


def solution(mesh):
    return jax.shard_map(
        per_device,
        mesh=mesh,
        in_specs=(P("orb", "grp", None), P(), P()),
        out_specs=P("orb", "grp", None),
        check_vma=False,
    )
```

```python
import functools
import math

import jax
import jax.numpy as jnp
from jax import lax
from jax.experimental import pallas as pl
from jax.experimental.pallas import tpu as pltpu
from jax.sharding import PartitionSpec as P

BOX = 32
PLANE = BOX * BOX
HALF = PLANE // 2
LANES = 128
SUBLANES = 8
TOP_EXP = 14.0
ORB_GRP = 64
CAP = 2
SCREEN = 0.25


def sine_table():
    counts = jnp.arange(BOX).astype(jnp.float32) + 1.0
    return jnp.sqrt(2.0 / (BOX + 1.0)) * jnp.sin(
        math.pi * counts[:, None] * counts[None, :] / (BOX + 1.0)
    )


def plane_modes(lanes):
    odd, place = lanes >> 9, lanes & (HALF - 1)
    y = place >> 4
    return y, 2 * (place & 15) + ((y + odd) & 1)


def green_rows():
    def level(index):
        return 2.0 - 2.0 * jnp.cos(math.pi * (index.astype(jnp.float32) + 1.0) / (BOX + 1.0))

    y, z = plane_modes(jnp.arange(PLANE, dtype=jnp.int32))
    x = level(jnp.arange(BOX, dtype=jnp.int32))
    return 1.0 / (x[:, None] + (level(y) + level(z))[None, :] + SCREEN)


def halves(value):
    high = value.astype(jnp.bfloat16)
    return high, (value - high.astype(jnp.float32)).astype(jnp.bfloat16)


def dot(a, b):
    return jnp.dot(a, b, preferred_element_type=jnp.float32)


def dot_back(a, b):
    return lax.dot_general(a, b, (((1,), (1,)), ((), ())), preferred_element_type=jnp.float32)


TABLES = 40


def plane_kernel(sine_ref, tables_hbm, table_ref, sems):
    lane = lax.broadcasted_iota(jnp.int32, (BOX, PLANE), 1)
    row = lax.broadcasted_iota(jnp.int32, (BOX, PLANE), 0)
    y, z = plane_modes(lane)
    by_y = jnp.where(y == row, 1.0, 0.0).astype(jnp.bfloat16)
    by_z = jnp.where(z == row, 1.0, 0.0).astype(jnp.bfloat16)
    parts = []
    rest = sine_ref[...]
    for _ in range(3):
        piece = rest.astype(jnp.bfloat16)
        parts.append(piece)
        rest = rest - piece.astype(jnp.float32)
    cols_y = dot(parts[0], by_y) + dot(parts[1], by_y) + dot(parts[2], by_y)
    cols_z = dot(parts[0], by_z) + dot(parts[1], by_z) + dot(parts[2], by_z)
    for m in range(BOX // 2):
        high, low = halves(cols_y[m : m + 1, :] * cols_z)
        part = slice(m * BOX, (m + 1) * BOX)
        for odd in range(2):
            modes = slice(odd * HALF, (odd + 1) * HALF)
            table_ref[2 * odd, part, :] = high[:, modes]
            table_ref[2 * odd + 1, part, :] = low[:, modes]
    copies = [
        pltpu.make_async_copy(table_ref.at[n], tables_hbm.at[n], sems.at[n]) for n in range(4)
    ]
    for copy in copies:
        copy.start()
    for copy in copies:
        copy.wait()


def plane_tables(sine):
    return pl.pallas_call(
        plane_kernel,
        out_shape=jax.ShapeDtypeStruct((TABLES, HALF, HALF), jnp.bfloat16),
        in_specs=[VMEM],
        out_specs=HBM,
        scratch_shapes=[
            pltpu.VMEM((4, HALF, HALF), jnp.bfloat16),
            pltpu.SemaphoreType.DMA((4,)),
        ],
        compiler_params=SOLVE_LIMIT,
        name="plane_tables",
    )(sine)


SIDE = 4
PAIR = 2


def pick_kernel(lists_ref, orbitals_ref, sent_out, *refs):
    local_outs, (columns, rows, picks_ref, own_ref, sems) = refs[:SIDE], refs[SIDE:]
    groups, pair_count = lists_ref.shape[1:]
    slots_each, rows_each = groups * CAP // SIDE**2, pair_count // SIDE**2
    each = slots_each + rows_each
    me = lax.axis_index("orb")
    x = lax.axis_index("grp") & (SIDE - 1)
    second = lists_ref[1].astype(jnp.float32)
    own_first = lists_ref[0, pl.ds(me, 1), :].astype(jnp.float32)
    own_slot = lists_ref[2, pl.ds(me, 1), :]
    group = lax.broadcasted_iota(jnp.int32, (groups, pair_count), 0)
    lane = lax.broadcasted_iota(jnp.int32, (groups, LANES), 1)
    table = jnp.zeros((groups, LANES), jnp.float32)
    for c in range(CAP):
        asked = jnp.where(lists_ref[2] == me * CAP + c, second, 0.0)
        named = jnp.where(own_slot == group * CAP + c, own_first, 0.0)
        table = jnp.where(lane == c, jnp.sum(asked, axis=1, keepdims=True), table)
        table = jnp.where(lane == CAP + c, jnp.sum(named, axis=1, keepdims=True), table)
    columns[...] = table.astype(jnp.int32)
    rows[...] = jnp.zeros_like(rows)
    rows[0:1, 0:pair_count] = own_first.astype(jnp.int32)
    copies = [
        pltpu.make_async_copy(columns, picks_ref, sems.at[0]),
        pltpu.make_async_copy(rows, own_ref, sems.at[1]),
    ]
    for copy in copies:
        copy.start()
    for copy in copies:
        copy.wait()
    for n in range(groups):
        for c in range(2 * CAP):
            sent_out[n * 2 * CAP + c] = orbitals_ref[picks_ref[n, c]]
    for step, out_ref in enumerate(local_outs):
        for y in range(SIDE):
            side = y * SIDE + ((x + step) & (SIDE - 1))
            for q in range(slots_each):
                pick = picks_ref[side * (slots_each // CAP) + q // CAP, q % CAP]
                out_ref[y * each + q] = orbitals_ref[pick]
            for q in range(rows_each):
                pick = own_ref[0, side * rows_each + q]
                out_ref[y * each + slots_each + q] = orbitals_ref[pick]


def turn_kernel(each, place_ref, *refs):
    came, gone = refs[:SIDE], refs[SIDE:]
    for step, out_ref in enumerate(gone):
        other = (place_ref[0] + step) & (SIDE - 1)
        for n, in_ref in enumerate(came):
            for q in range(each):
                out_ref[n * each + q] = in_ref[other * each + q]


def settle_kernel(each, place_ref, *refs):
    came, out_ref = refs[:SIDE], refs[SIDE]
    for far, in_ref in enumerate(came):
        y = (place_ref[0] - far) & (SIDE - 1)
        for near in range(SIDE):
            side = y * SIDE + ((place_ref[1] - near) & (SIDE - 1))
            for q in range(each):
                out_ref[side * each + q] = in_ref[near * each + q]


def pack_kernel(picks_ref, incoming_ref, out_ref):
    for n in range(out_ref.shape[0]):
        out_ref[n] = incoming_ref[picks_ref[n]]


def sum_kernel(share, depth, target_ref, terms_ref, out_ref, *sums):
    for held in sums:
        held[...] = jnp.zeros_like(held)
    chunks = PLANE // LANES
    block = depth * chunks
    each_x = terms_ref.shape[1] // depth
    for s in range(terms_ref.shape[0]):
        gains = jnp.exp2(-terms_ref[s, share * chunks : share * chunks + 1, :])
        for k in range(share):
            n = s * share + k
            held = sums[n % len(sums)]
            at = pl.ds(pl.multiple_of(target_ref[n] * block, block), block)
            term = [
                terms_ref[s, x * each_x + k * chunks : x * each_x + (k + 1) * chunks, :]
                for x in range(depth)
            ]
            held[at, :] = held[at, :] + jnp.concatenate(term, 0) * gains[:, k : k + 1]
    total = sums[0]
    total[...] = sum(held[...] for held in sums)
    for n in range(out_ref.shape[0]):
        for c in range(chunks):
            cells = pl.ds(n * block + c, depth, stride=chunks)
            out_ref[n, :, c * LANES : (c + 1) * LANES] = total[cells, :]


def same_pair():
    row = lax.broadcasted_iota(jnp.int32, (PAIR * BOX, PAIR * BOX), 0)
    col = lax.broadcasted_iota(jnp.int32, (PAIR * BOX, PAIR * BOX), 1)
    return row, col, (row >> 5) == (col >> 5)


def steps_along_x(moves_ref, at, back):
    row, col, same = same_pair()
    step = jnp.zeros(row.shape, jnp.int32)
    for k in range(PAIR):
        step = jnp.where((row >> 5) == k, moves_ref[at + k, 0], step)
    hit = (row == col + step) if back else (col == row + step)
    return jnp.where(same & hit, 1.0, 0.0).astype(jnp.bfloat16)


def moved(value, dy, dz):
    lane = lax.broadcasted_iota(jnp.int32, value.shape, 1)
    y, z = lane >> 5, lane & (BOX - 1)
    turned = pltpu.roll(value, (PLANE - (dy * BOX + dz)) & (PLANE - 1), 1)
    inside = (y + dy >= 0) & (y + dy < BOX) & (z + dz >= 0) & (z + dz < BOX)
    return jnp.where(inside, turned, 0.0)


def solve_kernel(
    homes,
    share,
    boxes_ref,
    local_ref,
    moves_hbm,
    sine_hbm,
    green_hbm,
    table_hbm,
    out_ref,
    first,
    second,
    held,
    moves_ref,
    sine_ref,
    green_ref,
    table_ref,
    sems,
):
    rows = share * BOX
    depth = boxes_ref.shape[1]
    sides = BOX // depth
    copies = [
        pltpu.make_async_copy(table_hbm.at[n], table_ref.at[n], sems.at[n]) for n in range(4)
    ] + [
        pltpu.make_async_copy(source, into, sems.at[4 + n])
        for n, (source, into) in enumerate(
            ((green_hbm, green_ref), (moves_hbm, moves_ref), (sine_hbm, sine_ref))
        )
    ]
    for n in (5, 6, 0, 1, 2, 3, 4):
        copies[n].start()
    for s in range(sides):
        for k in range(share):
            at = k * BOX + s * depth
            mine = second if k < homes else first
            q = s * share + (share - homes + k if k < homes else k - homes)
            mine[at : at + depth, :] = boxes_ref[q].astype(jnp.float32)
            other = first if k < homes else second
            other[at : at + depth, :] = local_ref[s * share + k].astype(jnp.float32)

    copies[5].wait()
    copies[6].wait()
    _, _, same = same_pair()
    wide = jnp.concatenate([jnp.concatenate([sine_ref[...]] * PAIR, 1)] * PAIR, 0)
    sine_high, sine_low = halves(jnp.where(same, wide, 0.0))
    three = jnp.concatenate([sine_high, sine_high, sine_low], 1)

    def along_x(value):
        high, low = halves(value)
        return dot(three, jnp.concatenate([high, low, high], 0))

    def mirrored(value):
        back = LANES - 1 - lax.broadcasted_iota(jnp.int32, (value.shape[0], LANES), 1)
        blocks = [value[:, n : n + LANES] for n in range(0, HALF, LANES)]
        return jnp.concatenate(
            [jnp.take_along_axis(block, back, axis=1) for block in reversed(blocks)], 1
        )

    def to_modes(value):
        near, far = value[:, :HALF], mirrored(value[:, HALF:])
        modes = []
        for n, part in ((0, near + far), (2, near - far)):
            high, low = halves(part)
            copies[n].wait()
            both = dot(jnp.concatenate([high, low], 0), table_ref[n])
            copies[n + 1].wait()
            modes.append(both[:rows] + both[rows:] + dot(high, table_ref[n + 1]))
        return jnp.concatenate(modes, 1)

    def to_cells(modes):
        even, odd = [], []
        for n, part, into in ((0, modes[:, :HALF], even), (2, modes[:, HALF:], odd)):
            high, low = halves(part)
            both = dot_back(jnp.concatenate([high, low], 0), table_ref[n])
            into.append(both[:rows] + both[rows:] + dot_back(high, table_ref[n + 1]))
        return jnp.concatenate([even[0] + odd[0], mirrored(even[0] - odd[0])], 1)

    charges = []
    for at in range(0, share, PAIR):
        turned = [
            moved(second[k * BOX : (k + 1) * BOX, :], moves_ref[k, 1], moves_ref[k, 2])
            for k in range(at, at + PAIR)
        ]
        ahead = steps_along_x(moves_ref, at, False)
        shifted = dot(ahead, jnp.concatenate(turned, 0).astype(jnp.bfloat16))
        part = slice(at * BOX, (at + PAIR) * BOX)
        if at < homes:
            second[part, :] = shifted
        charges.append(along_x(first[part, :] * shifted))
    modes = to_modes(jnp.concatenate(charges, 0))
    copies[4].wait()
    held[...] = to_cells(modes * jnp.concatenate([green_ref[...]] * share, 0))
    for at in range(0, share, PAIR):
        part = slice(at * BOX, (at + PAIR) * BOX)
        potential = along_x(held[part, :])
        if at < homes:
            held[part, :] = potential * second[part, :]
        else:
            high, low = halves(potential * first[part, :])
            back = steps_along_x(moves_ref, at, True)
            upright = dot(jnp.concatenate([back, back], 1), jnp.concatenate([high, low], 0))
            for k in range(PAIR):
                held[(at + k) * BOX : (at + k + 1) * BOX, :] = moved(
                    upright[k * BOX : (k + 1) * BOX],
                    -moves_ref[at + k, 1],
                    -moves_ref[at + k, 2],
                )
    each_x = out_ref.shape[0] // BOX
    lane = lax.broadcasted_iota(jnp.int32, (SUBLANES, LANES), 1)
    note = jnp.zeros((SUBLANES, LANES), jnp.float32)
    for k in range(share):
        value = held[k * BOX : (k + 1) * BOX, :]
        peak = jnp.max(jnp.abs(value), axis=(0, 1), keepdims=True)
        power = jnp.floor(TOP_EXP - jnp.log2(jnp.maximum(peak, 1e-30)))
        note = jnp.where(lane == k, power, note)
        value = value * jnp.exp2(power)
        for x in range(0, BOX, SUBLANES):
            for n in range(PLANE // LANES):
                row = x * each_x + k * (PLANE // LANES) + n
                out_ref[pl.ds(row, SUBLANES, stride=each_x), :] = value[
                    x : x + SUBLANES, n * LANES : (n + 1) * LANES
                ]
    for x in range(0, BOX, SUBLANES):
        for n in range(share * (PLANE // LANES), each_x):
            out_ref[pl.ds(x * each_x + n, SUBLANES, stride=each_x), :] = note


VMEM = pl.BlockSpec(memory_space=pltpu.VMEM)
SMEM = pl.BlockSpec(memory_space=pltpu.SMEM)
HBM = pl.BlockSpec(memory_space=pltpu.HBM)
ROWS_LIMIT = pltpu.CompilerParams(vmem_limit_bytes=20 << 20)
PICK_LIMIT = pltpu.CompilerParams(vmem_limit_bytes=66_900_000)
SOLVE_LIMIT = pltpu.CompilerParams(vmem_limit_bytes=46 << 20)


def rows_call(kernel, name, counts, in_specs, box, *args, scratch=(), limit=ROWS_LIMIT):
    out = tuple(jax.ShapeDtypeStruct((n, *box.shape[1:]), box.dtype) for n in counts)
    return pl.pallas_call(
        kernel,
        out_shape=out,
        in_specs=in_specs,
        out_specs=(VMEM,) * len(out),
        scratch_shapes=scratch,
        compiler_params=limit,
        name=name,
    )(*args)


def along(array, step, axis):
    pairs = []
    for n in range(SIDE * SIDE):
        at = list(divmod(n, SIDE))
        at[axis] = (at[axis] + step) % SIDE
        pairs.append((n, at[0] * SIDE + at[1]))
    return lax.ppermute(array, "grp", pairs)


def summed(target, terms, share, shape):
    scratch = pltpu.VMEM(((shape[0] + 1) * shape[1] * PLANE // LANES, LANES), terms.dtype)
    return pl.pallas_call(
        functools.partial(sum_kernel, share, shape[1]),
        out_shape=jax.ShapeDtypeStruct(shape, terms.dtype),
        in_specs=[SMEM, VMEM],
        out_specs=VMEM,
        scratch_shapes=[scratch] * 4,
        compiler_params=ROWS_LIMIT,
        name="sum_rows",
    )(target, terms)


def pair_terms(homes, share, boxes, local, moves, table, green, sine):
    cube = pltpu.VMEM((share * BOX, PLANE), jnp.float32)
    depth = boxes.shape[1]
    each_x = share * (PLANE // LANES) + SUBLANES // depth
    halves_type = pltpu.VMEM((4, HALF, HALF), jnp.bfloat16)
    return pl.pallas_call(
        functools.partial(solve_kernel, homes, share),
        out_shape=jax.ShapeDtypeStruct((BOX * each_x, LANES), jnp.float32),
        in_specs=[VMEM, VMEM, HBM, HBM, HBM, HBM],
        out_specs=VMEM,
        scratch_shapes=[
            cube,
            cube,
            cube,
            pltpu.SMEM(moves.shape, jnp.int32),
            pltpu.VMEM((BOX, BOX), jnp.float32),
            pltpu.VMEM((BOX, PLANE), jnp.float32),
            halves_type,
            pltpu.SemaphoreType.DMA((7,)),
        ],
        compiler_params=SOLVE_LIMIT,
        name="pair_terms",
    )(boxes, local, moves, sine, green, table)


def per_device(orbitals, pair_list, offsets):
    groups = lax.axis_size("orb")
    layers = lax.axis_size("grp")
    me = lax.axis_index("orb")
    region = lax.axis_index("grp")
    held, depth, plane = orbitals.shape
    slot_count = groups * CAP
    pair_count = pair_list.shape[1]
    rows_each = pair_count // layers
    slots_each = slot_count // layers
    swap = functools.partial(lax.all_to_all, split_axis=0, concat_axis=0, tiled=True)

    each = rows_each + slots_each
    side_rows = SIDE * each
    lists = jnp.transpose(pair_list, (2, 0, 1))
    outgoing, *local_rows = rows_call(
        pick_kernel,
        "pick_rows",
        (2 * slot_count,) + (side_rows,) * SIDE,
        [VMEM, VMEM],
        orbitals,
        lists,
        orbitals,
        scratch=[
            pltpu.VMEM((groups, LANES), jnp.int32),
            pltpu.VMEM((8, LANES), jnp.int32),
            pltpu.SMEM((groups, LANES), jnp.int32),
            pltpu.SMEM((8, LANES), jnp.int32),
            pltpu.SemaphoreType.DMA((2,)),
        ],
        limit=PICK_LIMIT,
    )
    incoming = swap(outgoing, "orb")

    place = jnp.stack([region // SIDE, region % SIDE])
    came = [local_rows[0]] + [along(local_rows[n], n, 1) for n in range(1, SIDE)]
    turned = rows_call(
        functools.partial(turn_kernel, each),
        "turn_rows",
        (side_rows,) * SIDE,
        [SMEM] + [VMEM] * SIDE,
        orbitals,
        place,
        *came,
    )
    (whole,) = rows_call(
        functools.partial(settle_kernel, each),
        "settle_rows",
        (layers * each,),
        [SMEM] + [VMEM] * SIDE,
        orbitals,
        place,
        turned[0],
        *(along(turned[n], n, 0) for n in range(1, SIDE)),
    )

    first_of, second_of, slot_of = lax.optimization_barrier(tuple(lists[n] for n in range(3)))
    is_me = jnp.arange(groups, dtype=jnp.int32)[:, None] == me
    first_local, second_local, slot = (
        jnp.sum(jnp.where(is_me, values, 0), axis=0) for values in (first_of, second_of, slot_of)
    )
    slot_ids = jnp.arange(slot_count, dtype=jnp.int32)
    wanted = me * CAP + jnp.arange(CAP, dtype=jnp.int32)
    asked = slot_of[:, None, :] == wanted[None, :, None]
    home_second = jnp.sum(jnp.where(asked, second_of[:, None, :], 0), axis=2).reshape(slot_count)
    home_valid = jnp.any(asked, axis=2).reshape(slot_count)
    target = jnp.concatenate(
        [
            jnp.where(home_valid, home_second, held).reshape(layers, slots_each),
            first_local.reshape(layers, rows_each),
        ],
        axis=1,
    ).reshape(-1)
    home_first = jnp.sum(jnp.where(asked, first_of[:, None, :], 0), axis=2).reshape(slot_count)
    from_rows = (slot // CAP * (2 * CAP) + slot % CAP).reshape(layers, rows_each)
    from_slots = (slot_ids // CAP * (2 * CAP) + CAP + slot_ids % CAP).reshape(layers, slots_each)
    from_incoming = jnp.concatenate([from_rows, from_slots], axis=1).reshape(-1)

    def part(values, count):
        return lax.dynamic_slice_in_dim(values, region * count, count, 0)

    first_ids = jnp.concatenate(
        [
            part(slot_ids // CAP * ORB_GRP + home_first, slots_each),
            part(me * ORB_GRP + first_local, rows_each),
        ]
    )
    second_ids = jnp.concatenate(
        [
            part(me * ORB_GRP + home_second, slots_each),
            part(slot // CAP * ORB_GRP + second_local, rows_each),
        ]
    )
    ids = jnp.arange(offsets.shape[0], dtype=jnp.int32)
    signs = (first_ids[:, None] == ids).astype(jnp.int32) - (
        second_ids[:, None] == ids
    ).astype(jnp.int32)
    moves = jnp.sum(signs[:, None, :] * offsets.T[None, :, :], axis=2)
    moves = jnp.pad(moves, ((0, -moves.shape[0] % 8), (0, LANES - moves.shape[1])))
    sine = sine_table()
    table = plane_tables(sine)
    green = green_rows()
    incoming, from_incoming, whole, moves, sine, table, green, target = (
        lax.optimization_barrier(
            (incoming, from_incoming, whole, moves, sine, table, green, target)
        )
    )

    (boxes,) = rows_call(
        pack_kernel,
        "pack_rows",
        (layers * each,),
        [SMEM, VMEM],
        orbitals,
        from_incoming,
        incoming,
    )
    boxes = swap(boxes, "grp")
    terms = pair_terms(slots_each, each, boxes, whole, moves, table, green, sine)
    terms = terms.reshape(layers, -1, LANES).astype(jnp.float16)
    terms = swap(terms, "grp").astype(jnp.float32)
    return summed(target, terms, each, orbitals.shape)


def solution(mesh):
    return jax.shard_map(
        per_device,
        mesh=mesh,
        in_specs=(P("orb", "grp", None), P(), P()),
        out_specs=P("orb", "grp", None),
        check_vma=False,
    )
```

```python
import functools
import math

import jax
import jax.numpy as jnp
from jax import lax
from jax.experimental import pallas as pl
from jax.experimental.pallas import tpu as pltpu
from jax.sharding import PartitionSpec as P

BOX = 32
PLANE = BOX * BOX
HALF = PLANE // 2
LANES = 128
SUBLANES = 8
TOP_EXP = 14.0
ORB_GRP = 64
CAP = 2
SCREEN = 0.25


def sine_table():
    counts = jnp.arange(BOX).astype(jnp.float32) + 1.0
    return jnp.sqrt(2.0 / (BOX + 1.0)) * jnp.sin(
        math.pi * counts[:, None] * counts[None, :] / (BOX + 1.0)
    )


def plane_modes(lanes):
    odd, place = lanes >> 9, lanes & (HALF - 1)
    y = place >> 4
    return y, 2 * (place & 15) + ((y + odd) & 1)


def green_rows():
    def level(index):
        return 2.0 - 2.0 * jnp.cos(math.pi * (index.astype(jnp.float32) + 1.0) / (BOX + 1.0))

    y, z = plane_modes(jnp.arange(PLANE, dtype=jnp.int32))
    x = level(jnp.arange(BOX, dtype=jnp.int32))
    return 1.0 / (x[:, None] + (level(y) + level(z))[None, :] + SCREEN)


def halves(value):
    high = value.astype(jnp.bfloat16)
    return high, (value - high.astype(jnp.float32)).astype(jnp.bfloat16)


def dot(a, b):
    return jnp.dot(a, b, preferred_element_type=jnp.float32)


def dot_back(a, b):
    return lax.dot_general(a, b, (((1,), (1,)), ((), ())), preferred_element_type=jnp.float32)


TABLES = 40


def plane_kernel(sine_ref, tables_hbm, table_ref, sems):
    lane = lax.broadcasted_iota(jnp.int32, (BOX, PLANE), 1)
    row = lax.broadcasted_iota(jnp.int32, (BOX, PLANE), 0)
    y, z = plane_modes(lane)
    by_y = jnp.where(y == row, 1.0, 0.0).astype(jnp.bfloat16)
    by_z = jnp.where(z == row, 1.0, 0.0).astype(jnp.bfloat16)
    parts = []
    rest = sine_ref[...]
    for _ in range(3):
        piece = rest.astype(jnp.bfloat16)
        parts.append(piece)
        rest = rest - piece.astype(jnp.float32)
    cols_y = dot(parts[0], by_y) + dot(parts[1], by_y) + dot(parts[2], by_y)
    cols_z = dot(parts[0], by_z) + dot(parts[1], by_z) + dot(parts[2], by_z)
    for m in range(BOX // 2):
        high, low = halves(cols_y[m : m + 1, :] * cols_z)
        part = slice(m * BOX, (m + 1) * BOX)
        for odd in range(2):
            modes = slice(odd * HALF, (odd + 1) * HALF)
            table_ref[2 * odd, part, :] = high[:, modes]
            table_ref[2 * odd + 1, part, :] = low[:, modes]
    copies = [
        pltpu.make_async_copy(table_ref.at[n], tables_hbm.at[n], sems.at[n]) for n in range(4)
    ]
    for copy in copies:
        copy.start()
    for copy in copies:
        copy.wait()


def plane_tables(sine):
    return pl.pallas_call(
        plane_kernel,
        out_shape=jax.ShapeDtypeStruct((TABLES, HALF, HALF), jnp.bfloat16),
        in_specs=[VMEM],
        out_specs=HBM,
        scratch_shapes=[
            pltpu.VMEM((4, HALF, HALF), jnp.bfloat16),
            pltpu.SemaphoreType.DMA((4,)),
        ],
        compiler_params=SOLVE_LIMIT,
        name="plane_tables",
    )(sine)


SIDE = 4
PAIR = 2


def pick_kernel(lists_ref, orbitals_ref, sent_out, *refs):
    local_outs, (columns, rows, picks_ref, own_ref, sems) = refs[:SIDE], refs[SIDE:]
    groups, pair_count = lists_ref.shape[1:]
    slots_each, rows_each = groups * CAP // SIDE**2, pair_count // SIDE**2
    each = slots_each + rows_each
    me = lax.axis_index("orb")
    x = lax.axis_index("grp") & (SIDE - 1)
    second = lists_ref[1].astype(jnp.float32)
    own_first = lists_ref[0, pl.ds(me, 1), :].astype(jnp.float32)
    own_slot = lists_ref[2, pl.ds(me, 1), :]
    group = lax.broadcasted_iota(jnp.int32, (groups, pair_count), 0)
    lane = lax.broadcasted_iota(jnp.int32, (groups, LANES), 1)
    table = jnp.zeros((groups, LANES), jnp.float32)
    for c in range(CAP):
        asked = jnp.where(lists_ref[2] == me * CAP + c, second, 0.0)
        named = jnp.where(own_slot == group * CAP + c, own_first, 0.0)
        table = jnp.where(lane == c, jnp.sum(asked, axis=1, keepdims=True), table)
        table = jnp.where(lane == CAP + c, jnp.sum(named, axis=1, keepdims=True), table)
    columns[...] = table.astype(jnp.int32)
    rows[...] = jnp.zeros_like(rows)
    rows[0:1, 0:pair_count] = own_first.astype(jnp.int32)
    copies = [
        pltpu.make_async_copy(columns, picks_ref, sems.at[0]),
        pltpu.make_async_copy(rows, own_ref, sems.at[1]),
    ]
    for copy in copies:
        copy.start()
    for copy in copies:
        copy.wait()
    for n in range(groups):
        for c in range(2 * CAP):
            sent_out[n * 2 * CAP + c] = orbitals_ref[picks_ref[n, c]]
    for step, out_ref in enumerate(local_outs):
        for y in range(SIDE):
            side = y * SIDE + ((x + step) & (SIDE - 1))
            for q in range(slots_each):
                pick = picks_ref[side * (slots_each // CAP) + q // CAP, q % CAP]
                out_ref[y * each + q] = orbitals_ref[pick]
            for q in range(rows_each):
                pick = own_ref[0, side * rows_each + q]
                out_ref[y * each + slots_each + q] = orbitals_ref[pick]


def turn_kernel(each, place_ref, *refs):
    came, gone = refs[:SIDE], refs[SIDE:]
    for step, out_ref in enumerate(gone):
        other = (place_ref[0] + step) & (SIDE - 1)
        for n, in_ref in enumerate(came):
            for q in range(each):
                out_ref[n * each + q] = in_ref[other * each + q]


def settle_kernel(each, place_ref, *refs):
    came, out_ref = refs[:SIDE], refs[SIDE]
    for far, in_ref in enumerate(came):
        y = (place_ref[0] - far) & (SIDE - 1)
        for near in range(SIDE):
            side = y * SIDE + ((place_ref[1] - near) & (SIDE - 1))
            for q in range(each):
                out_ref[side * each + q] = in_ref[near * each + q]


def pack_kernel(picks_ref, incoming_ref, out_ref):
    for n in range(out_ref.shape[0]):
        out_ref[n] = incoming_ref[picks_ref[n]]


def sum_kernel(share, depth, target_ref, terms_ref, out_ref, *sums):
    for held in sums:
        held[...] = jnp.zeros_like(held)
    chunks = PLANE // LANES
    block = depth * chunks
    each_x = terms_ref.shape[1] // depth
    for s in range(terms_ref.shape[0]):
        gains = jnp.exp2(-terms_ref[s, share * chunks : share * chunks + 1, :])
        for k in range(share):
            n = s * share + k
            held = sums[n % len(sums)]
            at = pl.ds(pl.multiple_of(target_ref[n] * block, block), block)
            term = [
                terms_ref[s, x * each_x + k * chunks : x * each_x + (k + 1) * chunks, :]
                for x in range(depth)
            ]
            held[at, :] = held[at, :] + jnp.concatenate(term, 0) * gains[:, k : k + 1]
    for n in range(out_ref.shape[0] // chunks):
        part = slice(n * chunks, (n + 1) * chunks)
        first_row = n // depth * block + n % depth
        out_ref[pl.ds(first_row, chunks, stride=depth), :] = sum(held[part, :] for held in sums)


def same_pair():
    row = lax.broadcasted_iota(jnp.int32, (PAIR * BOX, PAIR * BOX), 0)
    col = lax.broadcasted_iota(jnp.int32, (PAIR * BOX, PAIR * BOX), 1)
    return row, col, (row >> 5) == (col >> 5)


def steps_along_x(moves_ref, at, back):
    row, col, same = same_pair()
    step = jnp.zeros(row.shape, jnp.int32)
    for k in range(PAIR):
        step = jnp.where((row >> 5) == k, moves_ref[at + k, 0], step)
    hit = (row == col + step) if back else (col == row + step)
    return jnp.where(same & hit, 1.0, 0.0).astype(jnp.bfloat16)


def moved(value, dy, dz):
    lane = lax.broadcasted_iota(jnp.int32, value.shape, 1)
    y, z = lane >> 5, lane & (BOX - 1)
    turned = pltpu.roll(value, (PLANE - (dy * BOX + dz)) & (PLANE - 1), 1)
    inside = (y + dy >= 0) & (y + dy < BOX) & (z + dz >= 0) & (z + dz < BOX)
    return jnp.where(inside, turned, 0.0)


def solve_kernel(
    homes,
    share,
    boxes_ref,
    local_ref,
    moves_hbm,
    sine_hbm,
    green_hbm,
    table_hbm,
    out_ref,
    first,
    second,
    held,
    moves_ref,
    sine_ref,
    green_ref,
    table_ref,
    sems,
):
    rows = share * BOX
    depth = boxes_ref.shape[1]
    sides = BOX // depth
    copies = [
        pltpu.make_async_copy(table_hbm.at[n], table_ref.at[n], sems.at[n]) for n in range(4)
    ] + [
        pltpu.make_async_copy(source, into, sems.at[4 + n])
        for n, (source, into) in enumerate(
            ((green_hbm, green_ref), (moves_hbm, moves_ref), (sine_hbm, sine_ref))
        )
    ]
    for n in (5, 6, 0, 1, 2, 3, 4):
        copies[n].start()
    for s in range(sides):
        for k in range(share):
            at = k * BOX + s * depth
            mine = second if k < homes else first
            q = s * share + (share - homes + k if k < homes else k - homes)
            mine[at : at + depth, :] = boxes_ref[q].astype(jnp.float32)
            other = first if k < homes else second
            other[at : at + depth, :] = local_ref[s * share + k].astype(jnp.float32)

    copies[5].wait()
    copies[6].wait()
    _, _, same = same_pair()
    wide = jnp.concatenate([jnp.concatenate([sine_ref[...]] * PAIR, 1)] * PAIR, 0)
    sine_high, sine_low = halves(jnp.where(same, wide, 0.0))
    three = jnp.concatenate([sine_high, sine_high, sine_low], 1)

    def along_x(value):
        high, low = halves(value)
        return dot(three, jnp.concatenate([high, low, high], 0))

    def mirrored(value):
        back = LANES - 1 - lax.broadcasted_iota(jnp.int32, (value.shape[0], LANES), 1)
        blocks = [value[:, n : n + LANES] for n in range(0, HALF, LANES)]
        return jnp.concatenate(
            [jnp.take_along_axis(block, back, axis=1) for block in reversed(blocks)], 1
        )

    def to_modes(value):
        near, far = value[:, :HALF], mirrored(value[:, HALF:])
        modes = []
        for n, part in ((0, near + far), (2, near - far)):
            high, low = halves(part)
            copies[n].wait()
            both = dot(jnp.concatenate([high, low], 0), table_ref[n])
            copies[n + 1].wait()
            modes.append(both[:rows] + both[rows:] + dot(high, table_ref[n + 1]))
        return jnp.concatenate(modes, 1)

    def to_cells(modes):
        even, odd = [], []
        for n, part, into in ((0, modes[:, :HALF], even), (2, modes[:, HALF:], odd)):
            high, low = halves(part)
            both = dot_back(jnp.concatenate([high, low], 0), table_ref[n])
            into.append(both[:rows] + both[rows:] + dot_back(high, table_ref[n + 1]))
        return jnp.concatenate([even[0] + odd[0], mirrored(even[0] - odd[0])], 1)

    charges = []
    for at in range(0, share, PAIR):
        turned = [
            moved(second[k * BOX : (k + 1) * BOX, :], moves_ref[k, 1], moves_ref[k, 2])
            for k in range(at, at + PAIR)
        ]
        ahead = steps_along_x(moves_ref, at, False)
        shifted = dot(ahead, jnp.concatenate(turned, 0).astype(jnp.bfloat16))
        part = slice(at * BOX, (at + PAIR) * BOX)
        if at < homes:
            second[part, :] = shifted
        charges.append(along_x(first[part, :] * shifted))
    modes = to_modes(jnp.concatenate(charges, 0))
    copies[4].wait()
    held[...] = to_cells(modes * jnp.concatenate([green_ref[...]] * share, 0))
    for at in range(0, share, PAIR):
        part = slice(at * BOX, (at + PAIR) * BOX)
        potential = along_x(held[part, :])
        if at < homes:
            held[part, :] = potential * second[part, :]
        else:
            high, low = halves(potential * first[part, :])
            back = steps_along_x(moves_ref, at, True)
            upright = dot(jnp.concatenate([back, back], 1), jnp.concatenate([high, low], 0))
            for k in range(PAIR):
                held[(at + k) * BOX : (at + k + 1) * BOX, :] = moved(
                    upright[k * BOX : (k + 1) * BOX],
                    -moves_ref[at + k, 1],
                    -moves_ref[at + k, 2],
                )
    each_x = out_ref.shape[0] // BOX
    lane = lax.broadcasted_iota(jnp.int32, (SUBLANES, LANES), 1)
    note = jnp.zeros((SUBLANES, LANES), jnp.float32)
    for k in range(share):
        value = held[k * BOX : (k + 1) * BOX, :]
        peak = jnp.max(jnp.abs(value), axis=(0, 1), keepdims=True)
        power = jnp.floor(TOP_EXP - jnp.log2(jnp.maximum(peak, 1e-30)))
        note = jnp.where(lane == k, power, note)
        value = value * jnp.exp2(power)
        for x in range(0, BOX, SUBLANES):
            for n in range(PLANE // LANES):
                row = x * each_x + k * (PLANE // LANES) + n
                out_ref[pl.ds(row, SUBLANES, stride=each_x), :] = value[
                    x : x + SUBLANES, n * LANES : (n + 1) * LANES
                ]
    for x in range(0, BOX, SUBLANES):
        for n in range(share * (PLANE // LANES), each_x):
            out_ref[pl.ds(x * each_x + n, SUBLANES, stride=each_x), :] = note


VMEM = pl.BlockSpec(memory_space=pltpu.VMEM)
SMEM = pl.BlockSpec(memory_space=pltpu.SMEM)
HBM = pl.BlockSpec(memory_space=pltpu.HBM)
ROWS_LIMIT = pltpu.CompilerParams(vmem_limit_bytes=20 << 20)
PICK_LIMIT = pltpu.CompilerParams(vmem_limit_bytes=66_900_000)
SOLVE_LIMIT = pltpu.CompilerParams(vmem_limit_bytes=46 << 20)


def rows_call(kernel, name, counts, in_specs, box, *args, scratch=(), limit=ROWS_LIMIT):
    out = tuple(jax.ShapeDtypeStruct((n, *box.shape[1:]), box.dtype) for n in counts)
    return pl.pallas_call(
        kernel,
        out_shape=out,
        in_specs=in_specs,
        out_specs=(VMEM,) * len(out),
        scratch_shapes=scratch,
        compiler_params=limit,
        name=name,
    )(*args)


def along(array, step, axis):
    pairs = []
    for n in range(SIDE * SIDE):
        at = list(divmod(n, SIDE))
        at[axis] = (at[axis] + step) % SIDE
        pairs.append((n, at[0] * SIDE + at[1]))
    return lax.ppermute(array, "grp", pairs)


def summed(target, terms, share, shape):
    scratch = pltpu.VMEM(((shape[0] + 1) * shape[1] * PLANE // LANES, LANES), terms.dtype)
    return pl.pallas_call(
        functools.partial(sum_kernel, share, shape[1]),
        out_shape=jax.ShapeDtypeStruct((math.prod(shape) // LANES, LANES), terms.dtype),
        in_specs=[SMEM, VMEM],
        out_specs=VMEM,
        scratch_shapes=[scratch] * 4,
        compiler_params=ROWS_LIMIT,
        name="sum_rows",
    )(target, terms)


def pair_terms(homes, share, boxes, local, moves, table, green, sine):
    cube = pltpu.VMEM((share * BOX, PLANE), jnp.float32)
    depth = boxes.shape[1]
    each_x = share * (PLANE // LANES) + SUBLANES // depth
    halves_type = pltpu.VMEM((4, HALF, HALF), jnp.bfloat16)
    return pl.pallas_call(
        functools.partial(solve_kernel, homes, share),
        out_shape=jax.ShapeDtypeStruct((BOX * each_x, LANES), jnp.float32),
        in_specs=[VMEM, VMEM, HBM, HBM, HBM, HBM],
        out_specs=VMEM,
        scratch_shapes=[
            cube,
            cube,
            cube,
            pltpu.SMEM(moves.shape, jnp.int32),
            pltpu.VMEM((BOX, BOX), jnp.float32),
            pltpu.VMEM((BOX, PLANE), jnp.float32),
            halves_type,
            pltpu.SemaphoreType.DMA((7,)),
        ],
        compiler_params=SOLVE_LIMIT,
        name="pair_terms",
    )(boxes, local, moves, sine, green, table)


def per_device(orbitals, pair_list, offsets):
    groups = lax.axis_size("orb")
    layers = lax.axis_size("grp")
    me = lax.axis_index("orb")
    region = lax.axis_index("grp")
    held, depth, plane = orbitals.shape
    slot_count = groups * CAP
    pair_count = pair_list.shape[1]
    rows_each = pair_count // layers
    slots_each = slot_count // layers
    swap = functools.partial(lax.all_to_all, split_axis=0, concat_axis=0, tiled=True)

    each = rows_each + slots_each
    side_rows = SIDE * each
    lists = jnp.transpose(pair_list, (2, 0, 1))
    outgoing, *local_rows = rows_call(
        pick_kernel,
        "pick_rows",
        (2 * slot_count,) + (side_rows,) * SIDE,
        [VMEM, VMEM],
        orbitals,
        lists,
        orbitals,
        scratch=[
            pltpu.VMEM((groups, LANES), jnp.int32),
            pltpu.VMEM((8, LANES), jnp.int32),
            pltpu.SMEM((groups, LANES), jnp.int32),
            pltpu.SMEM((8, LANES), jnp.int32),
            pltpu.SemaphoreType.DMA((2,)),
        ],
        limit=PICK_LIMIT,
    )
    incoming = swap(outgoing, "orb")

    place = jnp.stack([region // SIDE, region % SIDE])
    came = [local_rows[0]] + [along(local_rows[n], n, 1) for n in range(1, SIDE)]
    turned = rows_call(
        functools.partial(turn_kernel, each),
        "turn_rows",
        (side_rows,) * SIDE,
        [SMEM] + [VMEM] * SIDE,
        orbitals,
        place,
        *came,
    )
    (whole,) = rows_call(
        functools.partial(settle_kernel, each),
        "settle_rows",
        (layers * each,),
        [SMEM] + [VMEM] * SIDE,
        orbitals,
        place,
        turned[0],
        *(along(turned[n], n, 0) for n in range(1, SIDE)),
    )

    first_of, second_of, slot_of = lax.optimization_barrier(tuple(lists[n] for n in range(3)))
    is_me = jnp.arange(groups, dtype=jnp.int32)[:, None] == me
    first_local, second_local, slot = (
        jnp.sum(jnp.where(is_me, values, 0), axis=0) for values in (first_of, second_of, slot_of)
    )
    slot_ids = jnp.arange(slot_count, dtype=jnp.int32)
    wanted = me * CAP + jnp.arange(CAP, dtype=jnp.int32)
    asked = slot_of[:, None, :] == wanted[None, :, None]
    home_second = jnp.sum(jnp.where(asked, second_of[:, None, :], 0), axis=2).reshape(slot_count)
    home_valid = jnp.any(asked, axis=2).reshape(slot_count)
    target = jnp.concatenate(
        [
            jnp.where(home_valid, home_second, held).reshape(layers, slots_each),
            first_local.reshape(layers, rows_each),
        ],
        axis=1,
    ).reshape(-1)
    home_first = jnp.sum(jnp.where(asked, first_of[:, None, :], 0), axis=2).reshape(slot_count)
    from_rows = (slot // CAP * (2 * CAP) + slot % CAP).reshape(layers, rows_each)
    from_slots = (slot_ids // CAP * (2 * CAP) + CAP + slot_ids % CAP).reshape(layers, slots_each)
    from_incoming = jnp.concatenate([from_rows, from_slots], axis=1).reshape(-1)

    def part(values, count):
        return lax.dynamic_slice_in_dim(values, region * count, count, 0)

    first_ids = jnp.concatenate(
        [
            part(slot_ids // CAP * ORB_GRP + home_first, slots_each),
            part(me * ORB_GRP + first_local, rows_each),
        ]
    )
    second_ids = jnp.concatenate(
        [
            part(me * ORB_GRP + home_second, slots_each),
            part(slot // CAP * ORB_GRP + second_local, rows_each),
        ]
    )
    ids = jnp.arange(offsets.shape[0], dtype=jnp.int32)
    signs = (first_ids[:, None] == ids).astype(jnp.int32) - (
        second_ids[:, None] == ids
    ).astype(jnp.int32)
    moves = jnp.sum(signs[:, None, :] * offsets.T[None, :, :], axis=2)
    moves = jnp.pad(moves, ((0, -moves.shape[0] % 8), (0, LANES - moves.shape[1])))
    sine = sine_table()
    table = plane_tables(sine)
    green = green_rows()
    incoming, from_incoming, whole, moves, sine, table, green, target = (
        lax.optimization_barrier(
            (incoming, from_incoming, whole, moves, sine, table, green, target)
        )
    )

    (boxes,) = rows_call(
        pack_kernel,
        "pack_rows",
        (layers * each,),
        [SMEM, VMEM],
        orbitals,
        from_incoming,
        incoming,
    )
    boxes = swap(boxes, "grp")
    terms = pair_terms(slots_each, each, boxes, whole, moves, table, green, sine)
    terms = terms.reshape(layers, -1, LANES).astype(jnp.float16)
    terms = swap(terms, "grp").astype(jnp.float32)
    action = summed(target, terms, each, orbitals.shape)
    action = action.reshape(held, plane // LANES, depth, LANES)
    return jnp.swapaxes(action, 1, 2).reshape(orbitals.shape)


def solution(mesh):
    return jax.shard_map(
        per_device,
        mesh=mesh,
        in_specs=(P("orb", "grp", None), P(), P()),
        out_specs=P("orb", "grp", None),
        check_vma=False,
    )
```
